32 devices in a mesh: row: 8 (over y, x, core), col: 4 (over z).
Axes of the slice: x: 2, y: 2, z: 4, core: 2. Of those that a mesh axis runs over, the one named last changes fastest.
Arguments:
- covariance: bfloat16 [16384, 16384], P('row', 'col'), may hold values from -0.12 to 0.6, as said below
- estimate: bfloat16 [16384, 16384], P('row', 'col'), may hold values from -2.3 to 12, as said below
- dual_var: bfloat16 [16384, 16384], P('row', 'col'), may hold values from -1.7 to 1.7, as said below
- start_basis: float32 [16384, 128], P('row'), may hold values from -6 to 6
Outputs:
- next_estimate: float32 [16384, 16384], P('row', 'col')
- next_dual: bfloat16 [16384, 16384], P('row', 'col')
The draws below stay inside these ranges and needn't reach their ends.
Inputs may be any that keep to these rules, and one draw needn't show every extreme that they name: `covariance`: symmetric. `estimate`: symmetric. `dual_var`: symmetric.
All inputs are finite; a program needn't handle non-finite values.
Results may differ from the reference program's by a relative error of at most 0.001.
Values sent between devices are 32-bit elements; how exact they have to be, the bound alone decides.
No kernel may reach another device: no remote copies, remote signals or barrier semaphores. Data moves between devices by JAX's collectives and lax.ppermute only.
A program may use at most 192 MiB of HBM per device.

```python
import jax
import jax.numpy as jnp
from jax import lax

P_SIZE = 16384
RANK = 128
ITERS = 1
NS_ITERS = 12
N_ROW = 8


def symmetric_part(key, spread):
    raw_draw = jax.random.truncated_normal(key, -4.0, 4.0, (P_SIZE, P_SIZE), jnp.float32)
    return (raw_draw + raw_draw.T) * (spread * 0.7071067811865476)


def on_diagonal():
    row_ids = lax.broadcasted_iota(jnp.int32, (P_SIZE, 1), 0)
    col_ids = lax.broadcasted_iota(jnp.int32, (1, P_SIZE), 1)
    return row_ids == col_ids


def draw_covariance(key, part):
    off_diag = symmetric_part(jax.random.fold_in(key, 11), 0.005)
    variances = jax.random.uniform(jax.random.fold_in(key, 12), (P_SIZE,), jnp.float32, 0.05, 0.15)
    matrix = jnp.where(on_diagonal(), variances[:, None], off_diag)
    return matrix.astype(jnp.bfloat16)


def draw_estimate(key, part):
    off_diag = symmetric_part(jax.random.fold_in(key, 21), 0.4)
    diagonal = jax.random.uniform(jax.random.fold_in(key, 22), (P_SIZE,), jnp.float32, 8.0, 12.0)
    return jnp.where(on_diagonal(), diagonal[:, None], off_diag).astype(jnp.bfloat16)


def draw_dual_var(key, part):
    return symmetric_part(jax.random.fold_in(key, 31), 0.3).astype(jnp.bfloat16)


def steps_of(stream_key, shape, split, least, top_value):
    def one(dim, blocks):
        steps = jax.random.uniform(jax.random.fold_in(jax.random.fold_in(stream_key, 6), dim), (blocks,), jnp.float32, least / len(split), top_value / len(split))
        return jnp.repeat(jnp.exp(steps), shape[dim] // blocks).reshape((-1,) + (1,) * (len(shape) - dim - 1))

    gain = one(*split[0])
    for cut in split[1:]:
        gain = gain * one(*cut)
    return gain


def bell_draw(stream_key, extent, scale, limit, cuts=(), kind=jnp.bfloat16):
    array = scale * jax.random.normal(stream_key, extent, jnp.float32)
    if cuts:
        array = array * steps_of(stream_key, extent, cuts, -0.22, 0.18)
    return jnp.clip(array, -limit, limit).astype(kind)


def setup_inputs(seed: int = 0) -> dict:
    keys = jax.random.split(jax.random.key(seed), 5)
    return {
        "covariance": draw_covariance(jax.random.fold_in(keys[4], 71), 0),
        "estimate": draw_estimate(jax.random.fold_in(keys[4], 71), 0),
        "dual_var": draw_dual_var(jax.random.fold_in(keys[4], 71), 0),
        "start_basis": bell_draw(keys[3], (P_SIZE, RANK), 1.0, 6.0, ((0, 8),), jnp.float32),
    }


penalty = 0.01
threshold = 0.2
base_level = 10.0
highest = lax.Precision.HIGHEST

def inner_product(left_side, right_side):
    return lax.dot_general(left_side.astype(jnp.float32), right_side.astype(jnp.float32), (((0,), (0,)), ((), ())), precision=highest, preferred_element_type=jnp.float32)

def normalize(mapped, gram_matrix):
    lower_factor = jnp.linalg.cholesky(gram_matrix)
    identity = jnp.eye(gram_matrix.shape[0], dtype=jnp.float32)
    inverse = lax.linalg.triangular_solve(lower_factor, identity, left_side=True, lower=True)
    return jnp.dot(mapped.astype(jnp.float32), inverse.T.astype(jnp.float32), precision=highest, preferred_element_type=jnp.float32)

def response_of(ritz_matrix):
    identity = jnp.eye(ritz_matrix.shape[0], dtype=jnp.float32)
    square = jnp.dot(ritz_matrix.astype(jnp.float32), ritz_matrix.astype(jnp.float32), precision=highest, preferred_element_type=jnp.float32) + 4.0 * penalty * identity
    frobenius = jnp.sqrt(jnp.sum(square * square))

    def newton(sweep_index, state_pair):
        iterate, partner = state_pair
        factor = 0.5 * (3.0 * identity - jnp.dot(partner.astype(jnp.float32), iterate.astype(jnp.float32), precision=highest, preferred_element_type=jnp.float32))
        return (jnp.dot(iterate.astype(jnp.float32), factor.astype(jnp.float32), precision=highest, preferred_element_type=jnp.float32), jnp.dot(factor.astype(jnp.float32), partner.astype(jnp.float32), precision=highest, preferred_element_type=jnp.float32))
    iterate, partner = lax.fori_loop(0, NS_ITERS, newton, (square / frobenius, identity))
    square_root = jnp.sqrt(frobenius) * iterate
    return (ritz_matrix + square_root) / (2.0 * penalty) - base_level * identity

def reference(covariance, estimate, dual_var, start_basis):
    shifted = penalty * (estimate.astype(jnp.float32) - dual_var.astype(jnp.float32)) - covariance.astype(jnp.float32)
    current = start_basis
    for sweep_index in range(ITERS):
        mapped = jnp.dot(shifted.astype(jnp.float32), current.astype(jnp.float32), precision=highest, preferred_element_type=jnp.float32)
        current = normalize(mapped, inner_product(mapped, mapped))
    product = jnp.dot(shifted.astype(jnp.float32), current.astype(jnp.float32), precision=highest, preferred_element_type=jnp.float32)
    raw_ritz = inner_product(current, product)
    ritz_matrix = 0.5 * (raw_ritz + raw_ritz.T)
    response = response_of(ritz_matrix)
    weighted = jnp.dot(current.astype(jnp.float32), response.astype(jnp.float32), precision=highest, preferred_element_type=jnp.float32)
    rows_block = P_SIZE // N_ROW

    def finish(block_index):
        row_start = block_index * rows_block
        left_rows = lax.dynamic_slice_in_dim(weighted, row_start, rows_block, 0)
        theta_tile = lax.dot_general(left_rows.astype(jnp.float32), current.astype(jnp.float32), (((1,), (1,)), ((), ())), precision=highest, preferred_element_type=jnp.float32)
        row_ids = row_start + lax.broadcasted_iota(jnp.int32, (rows_block, 1), 0)
        col_ids = lax.broadcasted_iota(jnp.int32, (1, P_SIZE), 1)
        theta_tile = theta_tile + jnp.where(row_ids == col_ids, base_level, 0.0)
        dual_rows = lax.dynamic_slice_in_dim(dual_var, row_start, rows_block, 0)
        mixture = theta_tile + dual_rows.astype(jnp.float32)
        clipped = jnp.clip(mixture, -threshold, threshold)
        return (mixture - clipped, clipped.astype(jnp.bfloat16))
    new_estimate, new_dual = lax.map(finish, jnp.arange(N_ROW, dtype=jnp.int32))
    return (new_estimate.reshape(P_SIZE, P_SIZE), new_dual.reshape(P_SIZE, P_SIZE))
```

```python
import functools

import jax
import jax.numpy as jnp
from jax import lax
from jax.experimental import pallas as pl
from jax.experimental.pallas import tpu as pltpu
from jax.sharding import PartitionSpec as P


NS_ITERS = 12


penalty = 0.01
threshold = 0.2
base_level = 10.0
highest = lax.Precision.HIGHEST


def from_root(value, axis, source):
    kept = jnp.where(lax.axis_index(axis) == source, value, 0).astype(value.dtype)
    return lax.psum(kept, axis)


def inner_product(left_side, right_side):
    return lax.dot_general(
        left_side,
        right_side,
        (((0,), (0,)), ((), ())),
        precision=highest,
        preferred_element_type=jnp.float32,
    )


def normalize(mapped, gram_matrix):
    lower_factor = jnp.linalg.cholesky(gram_matrix)
    identity = jnp.eye(gram_matrix.shape[0], dtype=jnp.float32)
    inverse = lax.linalg.triangular_solve(lower_factor, identity, left_side=True, lower=True)
    return jnp.dot(mapped, inverse.T, precision=highest, preferred_element_type=jnp.float32)


def response_of(ritz_matrix):
    identity = jnp.eye(ritz_matrix.shape[0], dtype=jnp.float32)
    square = (
        jnp.dot(ritz_matrix, ritz_matrix, precision=highest, preferred_element_type=jnp.float32)
        + 4.0 * penalty * identity
    )
    frobenius = jnp.sqrt(jnp.sum(square * square))

    def newton(sweep_index, state_pair):
        iterate, partner = state_pair
        factor = 0.5 * (
            3.0 * identity
            - jnp.dot(partner, iterate, precision=highest, preferred_element_type=jnp.float32)
        )
        return (
            jnp.dot(iterate, factor, precision=highest, preferred_element_type=jnp.float32),
            jnp.dot(factor, partner, precision=highest, preferred_element_type=jnp.float32),
        )

    iterate, partner = lax.fori_loop(0, NS_ITERS, newton, (square / frobenius, identity))
    square_root = jnp.sqrt(frobenius) * iterate
    return (ritz_matrix + square_root) / (2.0 * penalty) - base_level * identity


def column_basis(shifted, row_basis):
    partial_terms = lax.dot_general(
        shifted,
        row_basis,
        (((0,), (0,)), ((), ())),
        precision=highest,
        preferred_element_type=jnp.float32,
    )
    mapped = lax.psum(partial_terms, "row")
    gram_matrix = lax.psum(inner_product(mapped, mapped), "col")
    return normalize(mapped, gram_matrix)


def row_image(shifted, col_basis):
    local_terms = jnp.dot(shifted, col_basis, precision=highest, preferred_element_type=jnp.float32)
    return lax.psum(local_terms, "col")


def row_inner(left_side, right_side):
    return lax.psum(inner_product(left_side, right_side), "row")


def body(covariance, estimate, dual_var, start_basis):
    shifted = penalty * (
        estimate.astype(jnp.float32) - dual_var.astype(jnp.float32)
    ) - covariance.astype(jnp.float32)
    rows_tile = shifted.shape[0]
    cols_tile = shifted.shape[1]
    row_basis = start_basis
    col_basis = column_basis(shifted, row_basis)
    blocks_per_column = lax.axis_size("row") // lax.axis_size("col")
    row_index = lax.axis_index("row")
    own_block = lax.dynamic_slice_in_dim(
        col_basis, row_index % blocks_per_column * rows_tile, rows_tile, 0
    )
    row_basis = from_root(own_block, "col", row_index // blocks_per_column)
    product = row_image(shifted, col_basis)
    raw_ritz = row_inner(row_basis, product)
    ritz_matrix = 0.5 * (raw_ritz + raw_ritz.T)
    response = response_of(ritz_matrix)
    weighted = jnp.dot(row_basis, response, precision=highest, preferred_element_type=jnp.float32)
    theta_tile = lax.dot_general(
        weighted,
        col_basis,
        (((1,), (1,)), ((), ())),
        precision=highest,
        preferred_element_type=jnp.float32,
    )
    row_ids = row_index * rows_tile + lax.broadcasted_iota(jnp.int32, (rows_tile, 1), 0)
    col_ids = lax.axis_index("col") * cols_tile + lax.broadcasted_iota(jnp.int32, (1, cols_tile), 1)
    theta_tile = theta_tile + jnp.where(row_ids == col_ids, base_level, 0.0)
    mixture = theta_tile + dual_var.astype(jnp.float32)
    clipped = jnp.clip(mixture, -threshold, threshold)
    return (mixture - clipped, clipped.astype(jnp.bfloat16))


def pairs_of(n_row, n_col, send):
    pairs = []
    for row in range(n_row):
        for col in range(n_col):
            target = send(row, col)
            if target is not None:
                pairs.append((row * n_col + col, target[0] * n_col + target[1]))
    return pairs


def in_hbm(value):
    return pltpu.with_memory_space_constraint(value, pltpu.HBM)


def in_vmem(value):
    return pltpu.with_memory_space_constraint(value, pltpu.VMEM)


def split_two(value):
    high = value.astype(jnp.bfloat16)
    low = (value - high.astype(jnp.float32)).astype(jnp.bfloat16)
    return high, low


def contract(left_side, right_side, dims):
    return lax.dot_general(
        left_side, right_side, (dims, ((), ())), preferred_element_type=jnp.float32
    )


def image_kernel(order_ref, est_ref, dual_ref, cov_ref, basis_ref, part_ref, high_ref, held_ref, stack_ref):
    step = pl.program_id(0)
    rows, width = est_ref.shape
    rank = basis_ref.shape[1]

    @pl.when(step == 0)
    def _():
        high, low = split_two(basis_ref[...].T)
        stack_ref[:rank, :] = high
        stack_ref[rank:, :] = low

    depth = min(rows, 512)
    total = jnp.zeros((2 * rank, width), jnp.float32)
    extra = jnp.zeros((rank, width), jnp.float32)
    columns = pl.ds(pl.multiple_of(step * width, width), width)
    for start in range(0, rows, depth):
        span = slice(start, start + depth)
        dual_piece = dual_ref[span, :]
        shifted = penalty * (
            est_ref[span, :].astype(jnp.float32) - dual_piece.astype(jnp.float32)
        ) - cov_ref[span, :].astype(jnp.float32)
        high, low = split_two(shifted)
        high_ref[span, columns] = high
        held_ref[span, columns] = dual_piece
        total += contract(stack_ref[:, span], high, ((1,), (0,)))
        extra += contract(stack_ref[:rank, span], low, ((1,), (0,)))
    part_ref[0] = total[:rank] + total[rank:] + extra


def image_part(order, estimate, dual_var, covariance, basis, pieces, piece_width):
    rows = estimate.shape[0]
    rank = basis.shape[1]
    width = 256 if piece_width % 256 == 0 else 128
    per_piece = piece_width // width
    tile = pl.BlockSpec(
        (rows, width), lambda j, o: (0, o[j // per_piece] * per_piece + j % per_piece)
    )
    whole = pieces * piece_width
    return pl.pallas_call(
        image_kernel,
        out_shape=(
            jax.ShapeDtypeStruct((pieces, rank, piece_width), jnp.float32),
            pltpu.VMEM((rows, whole), jnp.bfloat16),
            pltpu.VMEM((rows, whole), jnp.bfloat16),
        ),
        grid_spec=pltpu.PrefetchScalarGridSpec(
            num_scalar_prefetch=1,
            grid=(pieces * per_piece,),
            in_specs=[tile, tile, tile, pl.BlockSpec((rows, rank), lambda j, o: (0, 0))],
            out_specs=[
                pl.BlockSpec((1, rank, width), lambda j, o: (j // per_piece, 0, j % per_piece)),
                pl.BlockSpec(memory_space=pltpu.VMEM),
                pl.BlockSpec(memory_space=pltpu.VMEM),
            ],
            scratch_shapes=[pltpu.VMEM((2 * rank, rows), jnp.bfloat16)],
        ),
        compiler_params=pltpu.CompilerParams(vmem_limit_bytes=14 * 2**20),
        name="image_part",
    )(order, in_hbm(estimate), in_hbm(dual_var), in_hbm(covariance), basis)


def product_kernel(high_ref, *refs, seeded):
    *piece_refs, out_ref, stack_ref = refs
    rank = out_ref.shape[1]
    rows = out_ref.shape[0]
    if seeded:
        *piece_refs, prior_ref = piece_refs
    width = piece_refs[0].shape[1]
    for index, piece_ref in enumerate(piece_refs):
        high, low = split_two(piece_ref[...])
        stack_ref[:rank, index * width : (index + 1) * width] = high
        stack_ref[rank:, index * width : (index + 1) * width] = low
    depth = min(rows, 256)
    for start in range(0, rows, depth):
        span = slice(start, start + depth)
        both = contract(high_ref[span, :], stack_ref[...], ((1,), (1,)))
        total = both[:, :rank] + both[:, rank:]
        out_ref[span, :] = prior_ref[span, :] + total if seeded else total


def product_part(high, pieces, prior=None):
    rows, whole = high.shape
    rank, width = pieces[0].shape
    seeded = prior is not None
    vmem = pl.BlockSpec(memory_space=pltpu.VMEM)
    return pl.pallas_call(
        functools.partial(product_kernel, seeded=seeded),
        out_shape=jax.ShapeDtypeStruct((rows, rank), jnp.float32),
        in_specs=[vmem] * (1 + len(pieces) + seeded),
        out_specs=vmem,
        scratch_shapes=[pltpu.VMEM((2 * rank, whole), jnp.bfloat16)],
        compiler_params=pltpu.CompilerParams(vmem_limit_bytes=12 * 2**20),
        name="product_part",
    )(in_vmem(high), *pieces, *([prior] * seeded))


def dot_three(left_side, right_side, dims=((1,), (0,))):
    left_high, left_low = split_two(left_side)
    right_high, right_low = split_two(right_side)
    return (
        contract(left_high, right_high, dims)
        + contract(left_low, right_high, dims)
        + contract(left_high, right_low, dims)
    )


def quadratic_kernel(where_ref, *refs):
    *piece_refs, product_ref, out_ref = refs
    width = piece_refs[0].shape[1]
    total = jnp.zeros(out_ref.shape, jnp.float32)
    for index, piece_ref in enumerate(piece_refs):
        start = pl.multiple_of(where_ref[index] * width, width)
        total += dot_three(piece_ref[...], product_ref[pl.ds(start, width), :])
    out_ref[...] = total


def quadratic(order, pieces, product):
    rank = product.shape[1]
    vmem = pl.BlockSpec(memory_space=pltpu.VMEM)
    return pl.pallas_call(
        quadratic_kernel,
        out_shape=jax.ShapeDtypeStruct((rank, rank), jnp.float32),
        in_specs=[pl.BlockSpec(memory_space=pltpu.SMEM)] + [vmem] * (len(pieces) + 1),
        out_specs=vmem,
        compiler_params=pltpu.CompilerParams(vmem_limit_bytes=8 * 2**20),
        name="quadratic",
    )(order, *pieces, product)


def gram_kernel(piece_ref, out_ref):
    out_ref[...] = dot_three(piece_ref[...], piece_ref[...], ((1,), (1,)))


def gram_of(piece):
    rank = piece.shape[0]
    vmem = pl.BlockSpec(memory_space=pltpu.VMEM)
    return pl.pallas_call(
        gram_kernel,
        out_shape=jax.ShapeDtypeStruct((rank, rank), jnp.float32),
        in_specs=[vmem],
        out_specs=vmem,
        compiler_params=pltpu.CompilerParams(vmem_limit_bytes=4 * 2**20),
        name="gram",
    )(piece)


def spread_row(band, index):
    return jnp.broadcast_to(band[index : index + 1, :], band.shape)


def spread_column(band, index):
    return jnp.broadcast_to(band[:, index : index + 1], band.shape)


def factor_kernel(gram_ref, out_ref):
    rank = gram_ref.shape[0]
    look = 4
    bands = rank // 8
    sublanes = lax.broadcasted_iota(jnp.int32, (8, rank), 0)
    lanes = lax.broadcasted_iota(jnp.int32, (8, rank), 1)
    left = [gram_ref[8 * i : 8 * i + 8, :] for i in range(bands)]
    right = [jnp.where(lanes == sublanes + 8 * i, 1.0, 0.0).astype(jnp.float32) for i in range(bands)]
    for start in range(0, rank, look):
        band, offset = start // 8, start % 8
        rows = [spread_row(left[band], offset + t) for t in range(look)]
        others = [spread_row(right[band], offset + t) for t in range(look)]
        small = [[spread_column(rows[t], start + u) for u in range(t + 1)] for t in range(look)]
        ratio = [[None] * look for _ in range(look)]
        scale = [None] * look
        for t in range(look):
            scale[t] = 1.0 / small[t][t]
            for v in range(t + 1, look):
                ratio[v][t] = small[v][t] * scale[t]
                for w in range(t + 1, v + 1):
                    small[v][w] = small[v][w] - ratio[v][t] * small[w][t]
                rows[v] = rows[v] - ratio[v][t] * rows[t]
                others[v] = others[v] - ratio[v][t] * others[t]
        for i in range(band, bands):
            columns = []
            for t in range(look):
                column = spread_column(left[i], start + t)
                for u in range(t):
                    column = column - ratio[t][u] * columns[u]
                columns.append(column)
            update, other = left[i], right[i]
            for t in range(look):
                amount = columns[t] * scale[t]
                update = update - amount * rows[t]
                other = other - amount * others[t]
            if i == band:
                final, final_other = left[i], right[i]
                for t in range(look):
                    root = lax.rsqrt(small[t][t])
                    final_other = jnp.where(sublanes == offset + t, others[t] * root, final_other)
                other = jnp.where(sublanes >= offset + look, other, final_other)
                update = jnp.where(sublanes >= offset + look, update, final)
            left[i], right[i] = update, other
    for i in range(bands):
        out_ref[8 * i : 8 * i + 8, :] = right[i]


def factor_of(gram):
    vmem = pl.BlockSpec(memory_space=pltpu.VMEM)
    return pl.pallas_call(
        factor_kernel,
        out_shape=jax.ShapeDtypeStruct(gram.shape, jnp.float32),
        in_specs=[vmem],
        out_specs=vmem,
        compiler_params=pltpu.CompilerParams(vmem_limit_bytes=4 * 2**20),
        name="factor",
    )(gram)


def core_kernel(small_ref, inverse_ref, out_ref):
    rank = small_ref.shape[0]
    row_ids = lax.broadcasted_iota(jnp.int32, (rank, rank), 0)
    col_ids = lax.broadcasted_iota(jnp.int32, (rank, rank), 1)
    identity = jnp.where(row_ids == col_ids, 1.0, 0.0).astype(jnp.float32)
    inverse = inverse_ref[...]
    raw = dot_three(dot_three(inverse, small_ref[...]), inverse, ((1,), (1,)))
    ritz = 0.5 * (raw + raw.T)
    square = dot_three(ritz, ritz) + 4.0 * penalty * identity
    frobenius = jnp.sqrt(jnp.sum(jnp.sum(square * square, axis=1, keepdims=True), axis=0, keepdims=True))

    def newton(_, pair):
        iterate, partner = pair
        factor = 0.5 * (3.0 * identity - dot_three(partner, iterate))
        return dot_three(iterate, factor), dot_three(factor, partner)

    iterate, _ = lax.fori_loop(0, NS_ITERS, newton, (square / frobenius, identity))
    root = jnp.sqrt(frobenius) * iterate
    response = (ritz + root) / (2.0 * penalty) - base_level * identity
    out_ref[...] = dot_three(dot_three(inverse, response, ((0,), (0,))), inverse)


def core_of(small, inverse):
    vmem = pl.BlockSpec(memory_space=pltpu.VMEM)
    return pl.pallas_call(
        core_kernel,
        out_shape=jax.ShapeDtypeStruct(small.shape, jnp.float32),
        in_specs=[vmem, vmem],
        out_specs=vmem,
        compiler_params=pltpu.CompilerParams(vmem_limit_bytes=8 * 2**20),
        name="core",
    )(small, inverse)


def finish_kernel(place_ref, left_ref, core_ref, right_ref, *refs, groups, pieces):
    *held_refs, est_ref, dual_ref, left_stack, right_twice, right_low = refs
    group = pl.program_id(0)
    piece = pl.program_id(1)
    height, width = est_ref.shape
    rank = core_ref.shape[0]

    @pl.when(group == 0)
    def _():
        weighted = dot_three(left_ref[0], core_ref[...], ((0,), (0,)))
        high, low = split_two(weighted)
        left_stack[piece, :, :rank] = high
        left_stack[piece, :, rank:] = low

    @pl.when(piece == 0)
    def _():
        high, low = split_two(right_ref[0])
        right_twice[:rank, :] = high
        right_twice[rank:, :] = high
        right_low[...] = low

    rows = pl.ds(pl.multiple_of(place_ref[groups + piece] * height, height), height)
    columns = pl.ds(pl.multiple_of(lax.rem(group, pieces) * width, width), width)
    held = held_refs[0][rows, columns]
    for index in range(1, len(held_refs)):
        held = jnp.where(group >= index * pieces, held_refs[index][rows, columns], held)
    theta = contract(left_stack[piece], right_twice[...], ((1,), (0,)))
    theta += contract(left_stack[piece, :, :rank], right_low[...], ((1,), (0,)))
    row_ids = place_ref[groups + 2 * pieces] + place_ref[groups + piece] * height
    col_ids = place_ref[groups + 2 * pieces + 1] + place_ref[group] * width
    row_ids = row_ids + lax.broadcasted_iota(jnp.int32, (height, 1), 0)
    col_ids = col_ids + lax.broadcasted_iota(jnp.int32, (1, width), 1)
    theta = theta + jnp.where(row_ids == col_ids, base_level, 0.0)
    mixture = theta + held.astype(jnp.float32)
    clipped = jnp.clip(mixture, -threshold, threshold)
    est_ref[...] = mixture - clipped
    dual_ref[...] = clipped.astype(jnp.bfloat16)


def finish(place, left, core, right, held):
    pieces, rank, width = left.shape
    groups = right.shape[0]
    rows = pieces * width
    columns = groups * width
    vmem = pl.BlockSpec(memory_space=pltpu.VMEM)
    tile = pl.BlockSpec((width, width), lambda g, a, p: (p[groups + a], p[g]))
    return pl.pallas_call(
        functools.partial(finish_kernel, groups=groups, pieces=pieces),
        out_shape=(
            jax.ShapeDtypeStruct((rows, columns), jnp.float32),
            jax.ShapeDtypeStruct((rows, columns), jnp.bfloat16),
        ),
        grid_spec=pltpu.PrefetchScalarGridSpec(
            num_scalar_prefetch=1,
            grid=(groups, pieces),
            in_specs=[
                pl.BlockSpec((1, rank, width), lambda g, a, p: (jnp.where(g == 0, a, 0), 0, 0)),
                vmem,
                pl.BlockSpec((1, rank, width), lambda g, a, p: (g, 0, 0)),
            ]
            + [vmem] * len(held),
            out_specs=[tile, tile],
            scratch_shapes=[
                pltpu.VMEM((pieces, width, 2 * rank), jnp.bfloat16),
                pltpu.VMEM((2 * rank, width), jnp.bfloat16),
                pltpu.VMEM((rank, width), jnp.bfloat16),
            ],
        ),
        compiler_params=pltpu.CompilerParams(vmem_limit_bytes=14 * 2**20),
        name="finish",
    )(place, left, core, right, *[in_vmem(part) for part in held])


def blocked_body(covariance, estimate, dual_var, start_basis):
    n_row, n_col = lax.axis_size("row"), lax.axis_size("col")
    lanes = n_row // n_col
    row_index, col_index = lax.axis_index("row"), lax.axis_index("col")
    lane, chip = row_index % lanes, row_index // lanes
    rows, columns = estimate.shape
    width = columns // n_row

    def across_lanes(value, step):
        route = [(r, r // lanes * lanes + (r % lanes ^ step)) for r in range(n_row)]
        return lax.ppermute(value, "row", route)

    def across_chips(value, step):
        route = [(r, (r // lanes ^ step) * lanes + r % lanes) for r in range(n_row)]
        return lax.ppermute(value, "row", route)

    def across_columns(value, step):
        return lax.ppermute(value, "col", [(c, c ^ step) for c in range(n_col)])

    def total_of(value):
        for move, count in ((across_lanes, lanes), (across_chips, n_col), (across_columns, n_col)):
            value = sum([move(value, step) for step in range(1, count)], value)
        return value

    def order_of(step):
        return jnp.stack([(lane ^ step) * n_col + (chip ^ s) for s in range(n_col)]).astype(jnp.int32)

    piece_rows = jnp.stack([col_index ^ a for a in range(n_col)]).astype(jnp.int32)
    orders = [order_of(step) for step in range(lanes)]
    corner = jnp.stack([row_index * rows, col_index * columns]).astype(jnp.int32)
    place = jnp.concatenate(orders + [piece_rows, piece_rows, corner])
    local = jnp.broadcast_to(chip == col_index, (8, 128)).astype(jnp.float32)
    orders, piece_rows, place, local = lax.optimization_barrier((orders, piece_rows, place, local))
    parts, highs, helds = {}, {}, {}
    for step in reversed(range(lanes)):
        parts[step], highs[step], helds[step] = image_part(
            orders[step], estimate, dual_var, covariance, start_basis, n_col, width
        )
    gathered = sum([across_lanes(parts[step], step) for step in range(1, lanes)], parts[0])
    own = sum([across_chips(gathered[s], s) for s in range(1, n_col)], gathered[0])
    half = [own] + [across_chips(own, s) for s in range(1, n_col)]
    left = []
    for a in range(n_col):
        route = [
            (r * n_col + c, (c * lanes + r % lanes) * n_col + (r // lanes ^ a))
            for r in range(n_row)
            for c in range(n_col)
            if r // lanes ^ a != c
        ]
        arrived = lax.ppermute(own, ("row", "col"), route)
        left.append(jnp.where(local[:1, :1] > 0.5, half[a], arrived))
    others = {0: half}
    for step in range(1, lanes):
        others[step] = [across_lanes(piece, step) for piece in half]
    inverse = factor_of(total_of(gram_of(own)))
    product = None
    for step in range(lanes):
        product = product_part(highs[step], others[step], product)
    small = total_of(quadratic(piece_rows, left, product))
    core = core_of(small, inverse)
    right = jnp.stack([piece for step in range(lanes) for piece in others[step]])
    return finish(place, jnp.stack(left), core, right, [helds[step] for step in range(lanes)])


def power_of_two(count):
    return count & (count - 1) == 0


def chosen_body(mesh):
    n_row, n_col = mesh.shape["row"], mesh.shape["col"]

    def pick(covariance, estimate, dual_var, start_basis):
        rows, columns = estimate.shape
        fits = n_row % n_col == 0 and power_of_two(n_row) and power_of_two(n_col)
        fits = fits and columns % (128 * n_row) == 0 and rows * n_row == columns * n_col
        fits = fits and start_basis.shape[1] % 128 == 0
        chosen = blocked_body if fits else body
        return chosen(covariance, estimate, dual_var, start_basis)

    return pick


def solution(mesh):
    return jax.shard_map(
        chosen_body(mesh),
        mesh=mesh,
        in_specs=(P("row", "col"), P("row", "col"), P("row", "col"), P("row", None)),
        out_specs=(P("row", "col"), P("row", "col")),
        check_vma=False,
    )
```

```python
import functools

import jax
import jax.numpy as jnp
from jax import lax
from jax.experimental import pallas as pl
from jax.experimental.pallas import tpu as pltpu
from jax.sharding import PartitionSpec as P


NS_ITERS = 12


penalty = 0.01
threshold = 0.2
base_level = 10.0
highest = lax.Precision.HIGHEST


def from_root(value, axis, source):
    kept = jnp.where(lax.axis_index(axis) == source, value, 0).astype(value.dtype)
    return lax.psum(kept, axis)


def inner_product(left_side, right_side):
    return lax.dot_general(
        left_side,
        right_side,
        (((0,), (0,)), ((), ())),
        precision=highest,
        preferred_element_type=jnp.float32,
    )


def normalize(mapped, gram_matrix):
    lower_factor = jnp.linalg.cholesky(gram_matrix)
    identity = jnp.eye(gram_matrix.shape[0], dtype=jnp.float32)
    inverse = lax.linalg.triangular_solve(lower_factor, identity, left_side=True, lower=True)
    return jnp.dot(mapped, inverse.T, precision=highest, preferred_element_type=jnp.float32)


def response_of(ritz_matrix):
    identity = jnp.eye(ritz_matrix.shape[0], dtype=jnp.float32)
    square = (
        jnp.dot(ritz_matrix, ritz_matrix, precision=highest, preferred_element_type=jnp.float32)
        + 4.0 * penalty * identity
    )
    frobenius = jnp.sqrt(jnp.sum(square * square))

    def newton(sweep_index, state_pair):
        iterate, partner = state_pair
        factor = 0.5 * (
            3.0 * identity
            - jnp.dot(partner, iterate, precision=highest, preferred_element_type=jnp.float32)
        )
        return (
            jnp.dot(iterate, factor, precision=highest, preferred_element_type=jnp.float32),
            jnp.dot(factor, partner, precision=highest, preferred_element_type=jnp.float32),
        )

    iterate, _ = lax.fori_loop(0, NS_ITERS, newton, (square / frobenius, identity))
    square_root = jnp.sqrt(frobenius) * iterate
    return (ritz_matrix + square_root) / (2.0 * penalty) - base_level * identity


def column_basis(shifted, row_basis):
    partial_terms = lax.dot_general(
        shifted,
        row_basis,
        (((0,), (0,)), ((), ())),
        precision=highest,
        preferred_element_type=jnp.float32,
    )
    mapped = lax.psum(partial_terms, "row")
    gram_matrix = lax.psum(inner_product(mapped, mapped), "col")
    return normalize(mapped, gram_matrix)


def row_image(shifted, col_basis):
    local_terms = jnp.dot(shifted, col_basis, precision=highest, preferred_element_type=jnp.float32)
    return lax.psum(local_terms, "col")


def row_inner(left_side, right_side):
    return lax.psum(inner_product(left_side, right_side), "row")


def body(covariance, estimate, dual_var, start_basis):
    shifted = penalty * (
        estimate.astype(jnp.float32) - dual_var.astype(jnp.float32)
    ) - covariance.astype(jnp.float32)
    rows_tile = shifted.shape[0]
    cols_tile = shifted.shape[1]
    row_basis = start_basis
    col_basis = column_basis(shifted, row_basis)
    blocks_per_column = lax.axis_size("row") // lax.axis_size("col")
    row_index = lax.axis_index("row")
    own_block = lax.dynamic_slice_in_dim(
        col_basis, row_index % blocks_per_column * rows_tile, rows_tile, 0
    )
    row_basis = from_root(own_block, "col", row_index // blocks_per_column)
    product = row_image(shifted, col_basis)
    raw_ritz = row_inner(row_basis, product)
    ritz_matrix = 0.5 * (raw_ritz + raw_ritz.T)
    response = response_of(ritz_matrix)
    weighted = jnp.dot(row_basis, response, precision=highest, preferred_element_type=jnp.float32)
    theta_tile = lax.dot_general(
        weighted,
        col_basis,
        (((1,), (1,)), ((), ())),
        precision=highest,
        preferred_element_type=jnp.float32,
    )
    row_ids = row_index * rows_tile + lax.broadcasted_iota(jnp.int32, (rows_tile, 1), 0)
    col_ids = lax.axis_index("col") * cols_tile + lax.broadcasted_iota(jnp.int32, (1, cols_tile), 1)
    theta_tile = theta_tile + jnp.where(row_ids == col_ids, base_level, 0.0)
    mixture = theta_tile + dual_var.astype(jnp.float32)
    clipped = jnp.clip(mixture, -threshold, threshold)
    return (mixture - clipped, clipped.astype(jnp.bfloat16))


def in_hbm(value):
    return pltpu.with_memory_space_constraint(value, pltpu.HBM)


def in_vmem(value):
    return pltpu.with_memory_space_constraint(value, pltpu.VMEM)


def split_two(value):
    high = value.astype(jnp.bfloat16)
    low = (value - high.astype(jnp.float32)).astype(jnp.bfloat16)
    return high, low


def contract(left_side, right_side, dims):
    return lax.dot_general(
        left_side, right_side, (dims, ((), ())), preferred_element_type=jnp.float32
    )


def image_kernel(order_ref, est_ref, dual_ref, cov_ref, basis_ref, *refs):
    part_ref, high_ref, held_ref, *more = refs
    step = pl.program_id(0)
    rows, width = est_ref.shape
    rank = part_ref.shape[1]
    stack_ref = basis_ref
    if more:
        stack_ref = more[0]

        @pl.when(step == 0)
        def _():
            high, low = split_two(basis_ref[...].T)
            stack_ref[:rank, :] = high
            stack_ref[rank:, :] = low

    depth = min(rows, 512)
    total = jnp.zeros((2 * rank, width), jnp.float32)
    extra = jnp.zeros((rank, width), jnp.float32)
    columns = pl.ds(pl.multiple_of(step * width, width), width)
    for start in range(0, rows, depth):
        span = slice(start, start + depth)
        dual_piece = dual_ref[span, :]
        shifted = penalty * (
            est_ref[span, :].astype(jnp.float32) - dual_piece.astype(jnp.float32)
        ) - cov_ref[span, :].astype(jnp.float32)
        high, low = split_two(shifted)
        high_ref[span, columns] = high
        held_ref[span, columns] = dual_piece
        total += contract(stack_ref[:, span], high, ((1,), (0,)))
        extra += contract(stack_ref[:rank, span], low, ((1,), (0,)))
    part_ref[0] = total[:rank] + total[rank:] + extra


def image_part(order, estimate, dual_var, covariance, basis, pieces, piece_width, first):
    rows = estimate.shape[0]
    rank = basis.shape[1] if first else basis.shape[0] // 2
    width = 256 if piece_width % 256 == 0 else 128
    per_piece = piece_width // width
    tile = pl.BlockSpec(
        (rows, width), lambda j, o: (0, o[j // per_piece] * per_piece + j % per_piece)
    )
    whole = pieces * piece_width
    vmem = pl.BlockSpec(memory_space=pltpu.VMEM)
    kept = pltpu.VMEM((rows, whole), jnp.bfloat16)
    stack = [jax.ShapeDtypeStruct((2 * rank, rows), jnp.bfloat16)] * first
    return pl.pallas_call(
        image_kernel,
        out_shape=(
            jax.ShapeDtypeStruct((pieces, rank, piece_width), jnp.float32), kept, kept, *stack
        ),
        grid_spec=pltpu.PrefetchScalarGridSpec(
            num_scalar_prefetch=1,
            grid=(pieces * per_piece,),
            in_specs=[tile, tile, tile, vmem],
            out_specs=[
                pl.BlockSpec((1, rank, width), lambda j, o: (j // per_piece, 0, j % per_piece)),
                vmem,
                vmem,
            ]
            + [vmem] * first,
        ),
        compiler_params=pltpu.CompilerParams(vmem_limit_bytes=14 * 2**20),
        name="image_part",
    )(order, in_hbm(estimate), in_hbm(dual_var), in_hbm(covariance), basis)


def product_kernel(*refs, counts, places, seeded):
    high_refs, refs = refs[: len(counts)], refs[len(counts) :]
    *piece_refs, out_ref, stack_ref = refs
    rows, rank = out_ref.shape
    if seeded:
        *piece_refs, prior_ref = piece_refs
    width = piece_refs[0].shape[1]
    for index, piece_ref in enumerate(piece_refs):
        high, low = split_two(piece_ref[...])
        stack_ref[:rank, index * width : (index + 1) * width] = high
        stack_ref[rank:, index * width : (index + 1) * width] = low
    depth = min(rows, 256)
    for start in range(0, rows, depth):
        span = slice(start, start + depth)
        both = jnp.zeros((depth, 2 * rank), jnp.float32)
        done = 0
        for high_ref, count, place in zip(high_refs, counts, places):
            there = slice(place * width, (place + count) * width)
            here = slice(done * width, (done + count) * width)
            both += contract(high_ref[span, there], stack_ref[:, here], ((1,), (1,)))
            done += count
        total = both[:, :rank] + both[:, rank:]
        out_ref[span, :] = prior_ref[span, :] + total if seeded else total


def product_part(highs, counts, places, pieces, prior=None):
    rows = highs[0].shape[0]
    rank, width = pieces[0].shape
    seeded = prior is not None
    vmem = pl.BlockSpec(memory_space=pltpu.VMEM)
    return pl.pallas_call(
        functools.partial(product_kernel, counts=counts, places=places, seeded=seeded),
        out_shape=jax.ShapeDtypeStruct((rows, rank), jnp.float32),
        in_specs=[vmem] * (len(highs) + len(pieces) + seeded),
        out_specs=vmem,
        scratch_shapes=[pltpu.VMEM((2 * rank, width * len(pieces)), jnp.bfloat16)],
        compiler_params=pltpu.CompilerParams(vmem_limit_bytes=12 * 2**20),
        name="product_part",
    )(*[in_vmem(high) for high in highs], *pieces, *([prior] * seeded))


def dot_three(left_side, right_side, dims=((1,), (0,))):
    left_high, left_low = split_two(left_side)
    right_high, right_low = split_two(right_side)
    return (
        contract(left_high, right_high, dims)
        + contract(left_low, right_high, dims)
        + contract(left_high, right_low, dims)
    )


def quadratic_kernel(where_ref, *refs):
    *piece_refs, product_ref, out_ref, small_ref, gram_ref = refs
    rank, width = piece_refs[0].shape
    small = jnp.zeros((rank, rank), jnp.float32)
    gram = jnp.zeros((rank, rank), jnp.float32)
    for index, piece_ref in enumerate(piece_refs):
        start = pl.multiple_of(where_ref[index] * width, width)
        small += dot_three(piece_ref[...], product_ref[pl.ds(start, width), :])
        gram += dot_three(piece_ref[...], piece_ref[...], ((1,), (1,)))
    small_ref[...] = small
    gram_ref[...] = gram
    lanes, _, share, _ = out_ref.shape
    for step in range(lanes):
        start = pl.multiple_of((where_ref[len(piece_refs)] ^ step) * share, share)
        out_ref[step, 0] = small_ref[pl.ds(start, share), :]
        out_ref[step, 1] = gram_ref[pl.ds(start, share), :]


def quadratic(order, pieces, product, lanes):
    rank = product.shape[1]
    vmem = pl.BlockSpec(memory_space=pltpu.VMEM)
    return pl.pallas_call(
        quadratic_kernel,
        out_shape=jax.ShapeDtypeStruct((lanes, 2, rank // lanes, rank), jnp.float32),
        in_specs=[pl.BlockSpec(memory_space=pltpu.SMEM)] + [vmem] * (len(pieces) + 1),
        out_specs=vmem,
        scratch_shapes=[pltpu.VMEM((rank, rank), jnp.float32)] * 2,
        compiler_params=pltpu.CompilerParams(vmem_limit_bytes=8 * 2**20),
        name="quadratic",
    )(order, *pieces, product)


def joined(where_ref, share_refs, whole_ref):
    share = share_refs[0].shape[0]
    lane = where_ref[where_ref.shape[0] - 1]
    for step, share_ref in enumerate(share_refs):
        start = pl.multiple_of((lane ^ step) * share, share)
        whole_ref[pl.ds(start, share), :] = share_ref[...]


def spread_row(band, index):
    return jnp.broadcast_to(band[index : index + 1, :], band.shape)


def spread_column(band, index):
    return jnp.broadcast_to(band[:, index : index + 1], band.shape)


def factor_kernel(where_ref, *refs):
    *share_refs, out_ref, gram_ref = refs
    joined(where_ref, share_refs, gram_ref)
    rank = gram_ref.shape[0]
    look = 4
    bands = rank // 8
    sublanes = lax.broadcasted_iota(jnp.int32, (8, rank), 0)
    lanes = lax.broadcasted_iota(jnp.int32, (8, rank), 1)
    left = [gram_ref[8 * i : 8 * i + 8, :] for i in range(bands)]
    right = [jnp.where(lanes == sublanes + 8 * i, 1.0, 0.0).astype(jnp.float32) for i in range(bands)]
    for start in range(0, rank, look):
        band, offset = start // 8, start % 8
        rows = [spread_row(left[band], offset + t) for t in range(look)]
        others = [spread_row(right[band], offset + t) for t in range(look)]
        small = [[spread_column(rows[t], start + u) for u in range(t + 1)] for t in range(look)]
        ratio = [[None] * look for _ in range(look)]
        scale = [None] * look
        for t in range(look):
            scale[t] = 1.0 / small[t][t]
            for v in range(t + 1, look):
                ratio[v][t] = small[v][t] * scale[t]
                for w in range(t + 1, v + 1):
                    small[v][w] = small[v][w] - ratio[v][t] * small[w][t]
                rows[v] = rows[v] - ratio[v][t] * rows[t]
                others[v] = others[v] - ratio[v][t] * others[t]
        for i in range(band, bands):
            columns = []
            for t in range(look):
                column = spread_column(left[i], start + t)
                for u in range(t):
                    column = column - ratio[t][u] * columns[u]
                columns.append(column)
            update, other = left[i], right[i]
            for t in range(look):
                amount = columns[t] * scale[t]
                update = update - amount * rows[t]
                other = other - amount * others[t]
            if i == band:
                final, final_other = left[i], right[i]
                for t in range(look):
                    root = lax.rsqrt(small[t][t])
                    final_other = jnp.where(sublanes == offset + t, others[t] * root, final_other)
                other = jnp.where(sublanes >= offset + look, other, final_other)
                update = jnp.where(sublanes >= offset + look, update, final)
            left[i], right[i] = update, other
    for i in range(bands):
        out_ref[8 * i : 8 * i + 8, :] = right[i]


def factor_of(order, shares):
    rank = shares[0].shape[1]
    vmem = pl.BlockSpec(memory_space=pltpu.VMEM)
    return pl.pallas_call(
        factor_kernel,
        out_shape=jax.ShapeDtypeStruct((rank, rank), jnp.float32),
        in_specs=[pl.BlockSpec(memory_space=pltpu.SMEM)] + [vmem] * len(shares),
        out_specs=vmem,
        scratch_shapes=[pltpu.VMEM((rank, rank), jnp.float32)],
        compiler_params=pltpu.CompilerParams(vmem_limit_bytes=4 * 2**20),
        name="factor",
    )(order, *shares)


def core_kernel(where_ref, inverse_ref, *refs):
    *share_refs, out_ref, small_ref = refs
    joined(where_ref, share_refs, small_ref)
    rank = small_ref.shape[0]
    row_ids = lax.broadcasted_iota(jnp.int32, (rank, rank), 0)
    col_ids = lax.broadcasted_iota(jnp.int32, (rank, rank), 1)
    identity = jnp.where(row_ids == col_ids, 1.0, 0.0).astype(jnp.float32)
    inverse = inverse_ref[...]
    raw = dot_three(dot_three(inverse, small_ref[...]), inverse, ((1,), (1,)))
    ritz = 0.5 * (raw + raw.T)
    square = dot_three(ritz, ritz) + 4.0 * penalty * identity
    frobenius = jnp.sqrt(jnp.sum(jnp.sum(square * square, axis=1, keepdims=True), axis=0, keepdims=True))

    def product(left_high, left_low, right_high, right_low):
        wide = jnp.concatenate([left_high, left_low], axis=1)
        twice = jnp.concatenate([right_high, right_high], axis=0)
        flat = ((1,), (0,))
        return contract(wide, twice, flat) + contract(left_high, right_low, flat)

    def newton(_, pair):
        high, low = split_two(pair)
        inner = product(high[rank:], low[rank:], high[:rank], low[:rank])
        factor = 0.5 * (3.0 * identity - inner)
        return product(high, low, *split_two(factor))

    pair = jnp.concatenate([square / frobenius, identity], axis=0)
    iterate = lax.fori_loop(0, NS_ITERS, newton, pair)[:rank]
    root = jnp.sqrt(frobenius) * iterate
    response = (ritz + root) / (2.0 * penalty) - base_level * identity
    out_ref[...] = dot_three(dot_three(inverse, response, ((0,), (0,))), inverse)


def core_of(order, inverse, shares):
    vmem = pl.BlockSpec(memory_space=pltpu.VMEM)
    return pl.pallas_call(
        core_kernel,
        out_shape=jax.ShapeDtypeStruct(inverse.shape, jnp.float32),
        in_specs=[pl.BlockSpec(memory_space=pltpu.SMEM)] + [vmem] * (1 + len(shares)),
        out_specs=vmem,
        scratch_shapes=[pltpu.VMEM(inverse.shape, jnp.float32)],
        compiler_params=pltpu.CompilerParams(vmem_limit_bytes=8 * 2**20),
        name="core",
    )(order, inverse, *shares)


def finish_kernel(place_ref, left_ref, core_ref, right_ref, *refs, groups, pieces, counts):
    *held_refs, est_ref, dual_ref, left_stack, right_twice, right_low = refs
    group = pl.program_id(0)
    piece = pl.program_id(1)
    height, width = est_ref.shape
    rank = core_ref.shape[0]

    @pl.when(group == 0)
    def _():
        weighted = dot_three(left_ref[0], core_ref[...], ((0,), (0,)))
        high, low = split_two(weighted)
        left_stack[piece, :, :rank] = high
        left_stack[piece, :, rank:] = low

    @pl.when(piece == 0)
    def _():
        high, low = split_two(right_ref[0])
        right_twice[:rank, :] = high
        right_twice[rank:, :] = high
        right_low[...] = low

    rows = pl.ds(pl.multiple_of(place_ref[groups + piece] * height, height), height)
    first, held = 0, None
    for held_ref, count in zip(held_refs, counts):
        at = jnp.clip(group - first, 0, count - 1)
        block = held_ref[rows, pl.ds(pl.multiple_of(at * width, width), width)]
        held = block if held is None else jnp.where(group >= first, block, held)
        first += count
    theta = contract(left_stack[piece], right_twice[...], ((1,), (0,)))
    theta += contract(left_stack[piece, :, :rank], right_low[...], ((1,), (0,)))
    row_ids = place_ref[groups + 2 * pieces] + place_ref[groups + piece] * height
    col_ids = place_ref[groups + 2 * pieces + 1] + place_ref[group] * width
    row_ids = row_ids + lax.broadcasted_iota(jnp.int32, (height, 1), 0)
    col_ids = col_ids + lax.broadcasted_iota(jnp.int32, (1, width), 1)
    theta = theta + jnp.where(row_ids == col_ids, base_level, 0.0)
    mixture = theta + held.astype(jnp.float32)
    clipped = jnp.clip(mixture, -threshold, threshold)
    est_ref[...] = mixture - clipped
    dual_ref[...] = clipped.astype(jnp.bfloat16)


def finish(place, left, core, right, held):
    pieces, rank, width = left.shape
    groups = right.shape[0]
    rows = pieces * width
    columns = groups * width
    vmem = pl.BlockSpec(memory_space=pltpu.VMEM)
    tile = pl.BlockSpec((width, width), lambda g, a, p: (p[groups + a], p[g]))
    return pl.pallas_call(
        functools.partial(
            finish_kernel, groups=groups, pieces=pieces, counts=[h.shape[1] // width for h in held]
        ),
        out_shape=(
            jax.ShapeDtypeStruct((rows, columns), jnp.float32),
            jax.ShapeDtypeStruct((rows, columns), jnp.bfloat16),
        ),
        grid_spec=pltpu.PrefetchScalarGridSpec(
            num_scalar_prefetch=1,
            grid=(groups, pieces),
            in_specs=[
                pl.BlockSpec((1, rank, width), lambda g, a, p: (jnp.where(g == 0, a, 0), 0, 0)),
                vmem,
                pl.BlockSpec((1, rank, width), lambda g, a, p: (g, 0, 0)),
            ]
            + [vmem] * len(held),
            out_specs=[tile, tile],
            scratch_shapes=[
                pltpu.VMEM((pieces, width, 2 * rank), jnp.bfloat16),
                pltpu.VMEM((2 * rank, width), jnp.bfloat16),
                pltpu.VMEM((rank, width), jnp.bfloat16),
            ],
        ),
        compiler_params=pltpu.CompilerParams(vmem_limit_bytes=14 * 2**20),
        name="finish",
    )(place, left, core, right, *[in_vmem(part) for part in held])


def blocked_body(*arguments):
    return blocked_steps(*arguments)


def blocked_steps(covariance, estimate, dual_var, start_basis):
    n_row, n_col = lax.axis_size("row"), lax.axis_size("col")
    lanes = n_row // n_col
    row_index, col_index = lax.axis_index("row"), lax.axis_index("col")
    lane, chip = row_index % lanes, row_index // lanes
    rows, columns = estimate.shape
    width = columns // n_row

    def across_lanes(value, step):
        route = [(r, r // lanes * lanes + (r % lanes ^ step)) for r in range(n_row)]
        return lax.ppermute(value, "row", route)

    def across_chips(value, step):
        route = [(r, (r // lanes ^ step) * lanes + r % lanes) for r in range(n_row)]
        return lax.ppermute(value, "row", route)

    def across_columns(value, step):
        return lax.ppermute(value, "col", [(c, c ^ step) for c in range(n_col)])

    def total_of(value, move, count):
        arrived = []
        for step in range(1, count):
            arrived.append(move(value, step))
        return sum(arrived, value)

    def block_at(step, s):
        return (lane ^ step) * n_col + (chip ^ s)

    calls = [[(step, s) for s in range(1, n_col)] for step in reversed(range(lanes))]
    calls.append([(step, 0) for step in reversed(range(lanes))])
    orders = [jnp.stack([block_at(*at) for at in call]).astype(jnp.int32) for call in calls]
    piece_rows = jnp.stack([col_index ^ a for a in range(n_col)]).astype(jnp.int32)
    corner = jnp.stack([row_index * rows, col_index * columns]).astype(jnp.int32)
    place = jnp.concatenate(orders + [piece_rows, piece_rows, corner])
    piece_rows = jnp.concatenate([piece_rows, lane.reshape(1).astype(jnp.int32)])
    local = jnp.broadcast_to(chip == col_index, (8, 128)).astype(jnp.float32)
    orders, piece_rows, place, local = lax.optimization_barrier((orders, piece_rows, place, local))

    part, high, held, basis = {}, [], [], in_hbm(start_basis)
    for index, call in enumerate(calls):
        if index == lanes:
            gathered = sum([part[step] for step in range(1, lanes)], part[0])
            gathered, orders[index] = lax.optimization_barrier((gathered, orders[index]))
        out = image_part(
            orders[index], estimate, dual_var, covariance, basis, len(call), width, index == 0
        )
        if index == 0:
            basis = out[3]
        high.append(out[1])
        held.append(out[2])
        step = call[0][0]
        if index < lanes:
            if step:
                part[step] = across_lanes(out[0], step)
            else:
                part[0] = out[0]
    last = out[0]
    own = last[lanes - 1]
    for index in range(lanes - 1):
        own = own + across_lanes(last[index], calls[-1][index][0])
    for s in range(1, n_col):
        arrived = across_chips(gathered[s - 1], s)
        own = own + arrived
    half = [own]
    for s in range(1, n_col):
        half.append(across_chips(own, s))
    arrivals = []
    for a in range(n_col):
        route = [
            (r * n_col + c, (c * lanes + r % lanes) * n_col + (r // lanes ^ a))
            for r in range(n_row)
            for c in range(n_col)
            if r // lanes ^ a != c
        ]
        arrivals.append(lax.ppermute(own, ("row", "col"), route))
    right = {(0, s): half[s] for s in range(n_col)}
    for step in range(1, lanes):
        for s in range(n_col):
            right[step, s] = across_lanes(half[s], step)
    product = None
    for step in range(lanes):
        at = lanes - 1 - step
        product = product_part(
            [high[at], high[lanes]],
            (n_col - 1, 1),
            (0, at),
            [right[step, s] for s in range(1, n_col)] + [right[step, 0]],
            product,
        )
    local, product = lax.optimization_barrier((local, product))
    left = [jnp.where(local[:1, :1] > 0.5, half[a], arrivals[a]) for a in range(n_col)]
    shares = quadratic(piece_rows, left, product, lanes)
    both = sum([across_lanes(shares[step], step) for step in range(1, lanes)], shares[0])
    both = total_of(both, across_chips, n_col)
    small, gram = lax.optimization_barrier((both[0], both[1]))

    def of_lanes(share):
        return [share] + [across_lanes(share, step) for step in range(1, lanes)]

    grams = of_lanes(gram)
    inverse = factor_of(piece_rows, grams)
    small = total_of(small, across_columns, n_col)
    smalls = of_lanes(small)
    core = core_of(piece_rows, inverse, smalls)
    right_all = jnp.stack([right[at] for call in calls for at in call])
    return finish(place, jnp.stack(left), core, right_all, held)


def power_of_two(count):
    return count & (count - 1) == 0


def chosen_body(mesh):
    n_row, n_col = mesh.shape["row"], mesh.shape["col"]

    def pick(covariance, estimate, dual_var, start_basis):
        rows, columns = estimate.shape
        fits = n_row % n_col == 0 and power_of_two(n_row) and power_of_two(n_col)
        fits = fits and columns % (128 * n_row) == 0 and rows * n_row == columns * n_col
        fits = fits and start_basis.shape[1] % 128 == 0
        chosen = blocked_body if fits else body
        return chosen(covariance, estimate, dual_var, start_basis)

    return pick


def solution(mesh):
    return jax.shard_map(
        chosen_body(mesh),
        mesh=mesh,
        in_specs=(P("row", "col"), P("row", "col"), P("row", "col"), P("row", None)),
        out_specs=(P("row", "col"), P("row", "col")),
        check_vma=False,
    )
```

```python
import functools

import jax
import jax.numpy as jnp
from jax import lax
from jax.experimental import pallas as pl
from jax.experimental.pallas import tpu as pltpu
from jax.sharding import PartitionSpec as P


NS_ITERS = 12


penalty = 0.01
threshold = 0.2
base_level = 10.0
highest = lax.Precision.HIGHEST


def from_root(value, axis, source):
    kept = jnp.where(lax.axis_index(axis) == source, value, 0).astype(value.dtype)
    return lax.psum(kept, axis)


def inner_product(left_side, right_side):
    return lax.dot_general(
        left_side,
        right_side,
        (((0,), (0,)), ((), ())),
        precision=highest,
        preferred_element_type=jnp.float32,
    )


def normalize(mapped, gram_matrix):
    lower_factor = jnp.linalg.cholesky(gram_matrix)
    identity = jnp.eye(gram_matrix.shape[0], dtype=jnp.float32)
    inverse = lax.linalg.triangular_solve(lower_factor, identity, left_side=True, lower=True)
    return jnp.dot(mapped, inverse.T, precision=highest, preferred_element_type=jnp.float32)


def response_of(ritz_matrix):
    identity = jnp.eye(ritz_matrix.shape[0], dtype=jnp.float32)
    square = (
        jnp.dot(ritz_matrix, ritz_matrix, precision=highest, preferred_element_type=jnp.float32)
        + 4.0 * penalty * identity
    )
    frobenius = jnp.sqrt(jnp.sum(square * square))

    def newton(sweep_index, state_pair):
        iterate, partner = state_pair
        factor = 0.5 * (
            3.0 * identity
            - jnp.dot(partner, iterate, precision=highest, preferred_element_type=jnp.float32)
        )
        return (
            jnp.dot(iterate, factor, precision=highest, preferred_element_type=jnp.float32),
            jnp.dot(factor, partner, precision=highest, preferred_element_type=jnp.float32),
        )

    iterate, _ = lax.fori_loop(0, NS_ITERS, newton, (square / frobenius, identity))
    square_root = jnp.sqrt(frobenius) * iterate
    return (ritz_matrix + square_root) / (2.0 * penalty) - base_level * identity


def column_basis(shifted, row_basis):
    partial_terms = lax.dot_general(
        shifted,
        row_basis,
        (((0,), (0,)), ((), ())),
        precision=highest,
        preferred_element_type=jnp.float32,
    )
    mapped = lax.psum(partial_terms, "row")
    gram_matrix = lax.psum(inner_product(mapped, mapped), "col")
    return normalize(mapped, gram_matrix)


def row_image(shifted, col_basis):
    local_terms = jnp.dot(shifted, col_basis, precision=highest, preferred_element_type=jnp.float32)
    return lax.psum(local_terms, "col")


def row_inner(left_side, right_side):
    return lax.psum(inner_product(left_side, right_side), "row")


def body(covariance, estimate, dual_var, start_basis):
    shifted = penalty * (
        estimate.astype(jnp.float32) - dual_var.astype(jnp.float32)
    ) - covariance.astype(jnp.float32)
    rows_tile = shifted.shape[0]
    cols_tile = shifted.shape[1]
    row_basis = start_basis
    col_basis = column_basis(shifted, row_basis)
    blocks_per_column = lax.axis_size("row") // lax.axis_size("col")
    row_index = lax.axis_index("row")
    own_block = lax.dynamic_slice_in_dim(
        col_basis, row_index % blocks_per_column * rows_tile, rows_tile, 0
    )
    row_basis = from_root(own_block, "col", row_index // blocks_per_column)
    product = row_image(shifted, col_basis)
    raw_ritz = row_inner(row_basis, product)
    ritz_matrix = 0.5 * (raw_ritz + raw_ritz.T)
    response = response_of(ritz_matrix)
    weighted = jnp.dot(row_basis, response, precision=highest, preferred_element_type=jnp.float32)
    theta_tile = lax.dot_general(
        weighted,
        col_basis,
        (((1,), (1,)), ((), ())),
        precision=highest,
        preferred_element_type=jnp.float32,
    )
    row_ids = row_index * rows_tile + lax.broadcasted_iota(jnp.int32, (rows_tile, 1), 0)
    col_ids = lax.axis_index("col") * cols_tile + lax.broadcasted_iota(jnp.int32, (1, cols_tile), 1)
    theta_tile = theta_tile + jnp.where(row_ids == col_ids, base_level, 0.0)
    mixture = theta_tile + dual_var.astype(jnp.float32)
    clipped = jnp.clip(mixture, -threshold, threshold)
    return (mixture - clipped, clipped.astype(jnp.bfloat16))


def in_hbm(value):
    return pltpu.with_memory_space_constraint(value, pltpu.HBM)


def in_vmem(value):
    return pltpu.with_memory_space_constraint(value, pltpu.VMEM)


def split_two(value):
    high = value.astype(jnp.bfloat16)
    low = (value - high.astype(jnp.float32)).astype(jnp.bfloat16)
    return high, low


def contract(left_side, right_side, dims):
    return lax.dot_general(
        left_side, right_side, (dims, ((), ())), preferred_element_type=jnp.float32
    )


def image_kernel(order_ref, est_ref, dual_ref, cov_ref, basis_ref, *refs):
    part_ref, high_ref, held_ref, *more = refs
    step = pl.program_id(0)
    rows, width = est_ref.shape
    rank = part_ref.shape[1]
    stack_ref = basis_ref
    if more:
        stack_ref = more[0]

        @pl.when(step == 0)
        def _():
            high, low = split_two(basis_ref[...].T)
            stack_ref[:rank, :] = high
            stack_ref[rank:, :] = low

    depth = min(rows, 512)
    total = jnp.zeros((2 * rank, width), jnp.float32)
    extra = jnp.zeros((rank, width), jnp.float32)
    columns = pl.ds(pl.multiple_of(step * width, width), width)
    for start in range(0, rows, depth):
        span = slice(start, start + depth)
        dual_piece = dual_ref[span, :]
        shifted = penalty * (
            est_ref[span, :].astype(jnp.float32) - dual_piece.astype(jnp.float32)
        ) - cov_ref[span, :].astype(jnp.float32)
        high, low = split_two(shifted)
        high_ref[span, columns] = high
        held_ref[span, columns] = dual_piece
        total += contract(stack_ref[:, span], high, ((1,), (0,)))
        extra += contract(stack_ref[:rank, span], low, ((1,), (0,)))
    part_ref[0] = total[:rank] + total[rank:] + extra


def image_part(order, estimate, dual_var, covariance, basis, pieces, piece_width, first):
    rows = estimate.shape[0]
    rank = basis.shape[1] if first else basis.shape[0] // 2
    width = 256 if piece_width % 256 == 0 else 128
    per_piece = piece_width // width
    tile = pl.BlockSpec(
        (rows, width), lambda j, o: (0, o[j // per_piece] * per_piece + j % per_piece)
    )
    whole = pieces * piece_width
    vmem = pl.BlockSpec(memory_space=pltpu.VMEM)
    kept = pltpu.VMEM((rows, whole), jnp.bfloat16)
    stack = [jax.ShapeDtypeStruct((2 * rank, rows), jnp.bfloat16)] * first
    return pl.pallas_call(
        image_kernel,
        out_shape=(
            jax.ShapeDtypeStruct((pieces, rank, piece_width), jnp.float32), kept, kept, *stack
        ),
        grid_spec=pltpu.PrefetchScalarGridSpec(
            num_scalar_prefetch=1,
            grid=(pieces * per_piece,),
            in_specs=[tile, tile, tile, vmem],
            out_specs=[
                pl.BlockSpec((1, rank, width), lambda j, o: (j // per_piece, 0, j % per_piece)),
                vmem,
                vmem,
            ]
            + [vmem] * first,
        ),
        compiler_params=pltpu.CompilerParams(vmem_limit_bytes=14 * 2**20),
        name="image_part",
    )(order, in_hbm(estimate), in_hbm(dual_var), in_hbm(covariance), basis)


def product_kernel(*refs, counts, places, seeded):
    high_refs, refs = refs[: len(counts)], refs[len(counts) :]
    *piece_refs, out_ref, stack_ref = refs
    rows, rank = out_ref.shape
    if seeded:
        *piece_refs, prior_ref = piece_refs
    width = piece_refs[0].shape[1]
    for index, piece_ref in enumerate(piece_refs):
        high, low = split_two(piece_ref[...])
        stack_ref[:rank, index * width : (index + 1) * width] = high
        stack_ref[rank:, index * width : (index + 1) * width] = low
    depth = min(rows, 256)
    for start in range(0, rows, depth):
        span = slice(start, start + depth)
        both = jnp.zeros((depth, 2 * rank), jnp.float32)
        done = 0
        for high_ref, count, place in zip(high_refs, counts, places):
            there = slice(place * width, (place + count) * width)
            here = slice(done * width, (done + count) * width)
            both += contract(high_ref[span, there], stack_ref[:, here], ((1,), (1,)))
            done += count
        total = both[:, :rank] + both[:, rank:]
        out_ref[span, :] = prior_ref[span, :] + total if seeded else total


def product_part(highs, counts, places, pieces, prior=None):
    rows = highs[0].shape[0]
    rank, width = pieces[0].shape
    seeded = prior is not None
    vmem = pl.BlockSpec(memory_space=pltpu.VMEM)
    return pl.pallas_call(
        functools.partial(product_kernel, counts=counts, places=places, seeded=seeded),
        out_shape=jax.ShapeDtypeStruct((rows, rank), jnp.float32),
        in_specs=[vmem] * (len(highs) + len(pieces) + seeded),
        out_specs=vmem,
        scratch_shapes=[pltpu.VMEM((2 * rank, width * len(pieces)), jnp.bfloat16)],
        compiler_params=pltpu.CompilerParams(vmem_limit_bytes=12 * 2**20),
        name="product_part",
    )(*[in_vmem(high) for high in highs], *pieces, *([prior] * seeded))


def dot_three(left_side, right_side, dims=((1,), (0,))):
    left_high, left_low = split_two(left_side)
    right_high, right_low = split_two(right_side)
    return (
        contract(left_high, right_high, dims)
        + contract(left_low, right_high, dims)
        + contract(left_high, right_low, dims)
    )


def quadratic_kernel(where_ref, *refs):
    *piece_refs, product_ref, out_ref, small_ref, gram_ref = refs
    rank, width = piece_refs[0].shape
    small = jnp.zeros((rank, rank), jnp.float32)
    gram = jnp.zeros((rank, rank), jnp.float32)
    for index, piece_ref in enumerate(piece_refs):
        start = pl.multiple_of(where_ref[index] * width, width)
        small += dot_three(piece_ref[...], product_ref[pl.ds(start, width), :])
        gram += dot_three(piece_ref[...], piece_ref[...], ((1,), (1,)))
    small_ref[...] = small
    gram_ref[...] = gram
    lanes, _, share, _ = out_ref.shape
    for step in range(lanes):
        start = pl.multiple_of((where_ref[len(piece_refs)] ^ step) * share, share)
        out_ref[step, 0] = small_ref[pl.ds(start, share), :]
        out_ref[step, 1] = gram_ref[pl.ds(start, share), :]


def quadratic(order, pieces, product, lanes):
    rank = product.shape[1]
    vmem = pl.BlockSpec(memory_space=pltpu.VMEM)
    return pl.pallas_call(
        quadratic_kernel,
        out_shape=jax.ShapeDtypeStruct((lanes, 2, rank // lanes, rank), jnp.float32),
        in_specs=[pl.BlockSpec(memory_space=pltpu.SMEM)] + [vmem] * (len(pieces) + 1),
        out_specs=vmem,
        scratch_shapes=[pltpu.VMEM((rank, rank), jnp.float32)] * 2,
        compiler_params=pltpu.CompilerParams(vmem_limit_bytes=8 * 2**20),
        name="quadratic",
    )(order, *pieces, product)


def joined(where_ref, share_refs, whole_ref):
    share = share_refs[0].shape[0]
    lane = where_ref[where_ref.shape[0] - 1]
    for step, share_ref in enumerate(share_refs):
        start = pl.multiple_of((lane ^ step) * share, share)
        whole_ref[pl.ds(start, share), :] = share_ref[...]


def spread_row(band, index):
    return jnp.broadcast_to(band[index : index + 1, :], band.shape)


def spread_column(band, index):
    return jnp.broadcast_to(band[:, index : index + 1], band.shape)


def factor_kernel(where_ref, *refs):
    *share_refs, out_ref, gram_ref = refs
    joined(where_ref, share_refs, gram_ref)
    rank = gram_ref.shape[0]
    look = 8
    bands = rank // 8
    sublanes = lax.broadcasted_iota(jnp.int32, (8, rank), 0)
    lanes = lax.broadcasted_iota(jnp.int32, (8, rank), 1)
    left = [gram_ref[8 * i : 8 * i + 8, :] for i in range(bands)]
    right = [jnp.where(lanes == sublanes + 8 * i, 1.0, 0.0).astype(jnp.float32) for i in range(bands)]
    for start in range(0, rank, look):
        band, offset = start // 8, start % 8
        rows = [spread_row(left[band], offset + t) for t in range(look)]
        others = [spread_row(right[band], offset + t) for t in range(look)]
        small = [[spread_column(rows[t], start + u) for u in range(t + 1)] for t in range(look)]
        ratio = [[None] * look for _ in range(look)]
        scale = [None] * look
        for t in range(look):
            scale[t] = 1.0 / small[t][t]
            for v in range(t + 1, look):
                ratio[v][t] = small[v][t] * scale[t]
                for w in range(t + 1, v + 1):
                    small[v][w] = small[v][w] - ratio[v][t] * small[w][t]
                rows[v] = rows[v] - ratio[v][t] * rows[t]
                others[v] = others[v] - ratio[v][t] * others[t]
        for i in range(band, bands):
            columns = []
            for t in range(look):
                column = spread_column(left[i], start + t)
                for u in range(t):
                    column = column - ratio[t][u] * columns[u]
                columns.append(column)
            update, other = left[i], right[i]
            for t in range(look):
                amount = columns[t] * scale[t]
                update = update - amount * rows[t]
                other = other - amount * others[t]
            if i == band:
                final, final_other = left[i], right[i]
                for t in range(look):
                    root = lax.rsqrt(small[t][t])
                    final_other = jnp.where(sublanes == offset + t, others[t] * root, final_other)
                other = jnp.where(sublanes >= offset + look, other, final_other)
                update = jnp.where(sublanes >= offset + look, update, final)
            left[i], right[i] = update, other
    for i in range(bands):
        out_ref[8 * i : 8 * i + 8, :] = right[i]


def factor_of(order, shares):
    rank = shares[0].shape[1]
    vmem = pl.BlockSpec(memory_space=pltpu.VMEM)
    return pl.pallas_call(
        factor_kernel,
        out_shape=jax.ShapeDtypeStruct((rank, rank), jnp.float32),
        in_specs=[pl.BlockSpec(memory_space=pltpu.SMEM)] + [vmem] * len(shares),
        out_specs=vmem,
        scratch_shapes=[pltpu.VMEM((rank, rank), jnp.float32)],
        compiler_params=pltpu.CompilerParams(vmem_limit_bytes=4 * 2**20),
        name="factor",
    )(order, *shares)


def core_kernel(where_ref, inverse_ref, *refs):
    *share_refs, out_ref, small_ref = refs
    joined(where_ref, share_refs, small_ref)
    rank = small_ref.shape[0]
    row_ids = lax.broadcasted_iota(jnp.int32, (rank, rank), 0)
    col_ids = lax.broadcasted_iota(jnp.int32, (rank, rank), 1)
    identity = jnp.where(row_ids == col_ids, 1.0, 0.0).astype(jnp.float32)
    inverse = inverse_ref[...]
    raw = dot_three(dot_three(inverse, small_ref[...]), inverse, ((1,), (1,)))
    ritz = 0.5 * (raw + raw.T)
    square = dot_three(ritz, ritz) + 4.0 * penalty * identity
    frobenius = jnp.sqrt(jnp.sum(jnp.sum(square * square, axis=1, keepdims=True), axis=0, keepdims=True))

    def product(left_high, left_low, right_high, right_low):
        wide = jnp.concatenate([left_high, left_low], axis=1)
        twice = jnp.concatenate([right_high, right_high], axis=0)
        flat = ((1,), (0,))
        return contract(wide, twice, flat) + contract(left_high, right_low, flat)

    def newton(_, pair):
        iterate, partner = pair
        iterate_parts, partner_parts = split_two(iterate), split_two(partner)
        factor = 0.5 * (3.0 * identity - product(*partner_parts, *iterate_parts))
        factor_parts = split_two(factor)
        return product(*iterate_parts, *factor_parts), product(*factor_parts, *partner_parts)

    iterate, _ = lax.fori_loop(0, NS_ITERS, newton, (square / frobenius, identity))
    root = jnp.sqrt(frobenius) * iterate
    response = (ritz + root) / (2.0 * penalty) - base_level * identity
    out_ref[...] = dot_three(dot_three(inverse, response, ((0,), (0,))), inverse)


def core_of(order, inverse, shares):
    vmem = pl.BlockSpec(memory_space=pltpu.VMEM)
    return pl.pallas_call(
        core_kernel,
        out_shape=jax.ShapeDtypeStruct(inverse.shape, jnp.float32),
        in_specs=[pl.BlockSpec(memory_space=pltpu.SMEM)] + [vmem] * (1 + len(shares)),
        out_specs=vmem,
        scratch_shapes=[pltpu.VMEM(inverse.shape, jnp.float32)],
        compiler_params=pltpu.CompilerParams(vmem_limit_bytes=8 * 2**20),
        name="core",
    )(order, inverse, *shares)


def finish_kernel(place_ref, left_ref, core_ref, right_ref, *refs, groups, pieces, counts):
    *held_refs, est_ref, dual_ref, left_stack, right_twice, right_low = refs
    group = pl.program_id(0)
    piece = pl.program_id(1)
    height, width = est_ref.shape
    rank = core_ref.shape[0]

    @pl.when(group == 0)
    def _():
        weighted = dot_three(left_ref[0], core_ref[...], ((0,), (0,)))
        high, low = split_two(weighted)
        left_stack[piece, :, :rank] = high
        left_stack[piece, :, rank:] = low

    @pl.when(piece == 0)
    def _():
        high, low = split_two(right_ref[0])
        right_twice[:rank, :] = high
        right_twice[rank:, :] = high
        right_low[...] = low

    rows = pl.ds(pl.multiple_of(place_ref[groups + piece] * height, height), height)
    first, held = 0, None
    for held_ref, count in zip(held_refs, counts):
        at = jnp.clip(group - first, 0, count - 1)
        block = held_ref[rows, pl.ds(pl.multiple_of(at * width, width), width)]
        held = block if held is None else jnp.where(group >= first, block, held)
        first += count
    theta = contract(left_stack[piece], right_twice[...], ((1,), (0,)))
    theta += contract(left_stack[piece, :, :rank], right_low[...], ((1,), (0,)))
    row_ids = place_ref[groups + 2 * pieces] + place_ref[groups + piece] * height
    col_ids = place_ref[groups + 2 * pieces + 1] + place_ref[group] * width
    row_ids = row_ids + lax.broadcasted_iota(jnp.int32, (height, 1), 0)
    col_ids = col_ids + lax.broadcasted_iota(jnp.int32, (1, width), 1)
    theta = theta + jnp.where(row_ids == col_ids, base_level, 0.0)
    mixture = theta + held.astype(jnp.float32)
    clipped = jnp.clip(mixture, -threshold, threshold)
    est_ref[...] = mixture - clipped
    dual_ref[...] = clipped.astype(jnp.bfloat16)


def finish(place, left, core, right, held):
    pieces, rank, width = left.shape
    groups = right.shape[0]
    rows = pieces * width
    columns = groups * width
    vmem = pl.BlockSpec(memory_space=pltpu.VMEM)
    tile = pl.BlockSpec((width, width), lambda g, a, p: (p[groups + a], p[g]))
    return pl.pallas_call(
        functools.partial(
            finish_kernel, groups=groups, pieces=pieces, counts=[h.shape[1] // width for h in held]
        ),
        out_shape=(
            jax.ShapeDtypeStruct((rows, columns), jnp.float32),
            jax.ShapeDtypeStruct((rows, columns), jnp.bfloat16),
        ),
        grid_spec=pltpu.PrefetchScalarGridSpec(
            num_scalar_prefetch=1,
            grid=(groups, pieces),
            in_specs=[
                pl.BlockSpec((1, rank, width), lambda g, a, p: (jnp.where(g == 0, a, 0), 0, 0)),
                vmem,
                pl.BlockSpec((1, rank, width), lambda g, a, p: (g, 0, 0)),
            ]
            + [vmem] * len(held),
            out_specs=[tile, tile],
            scratch_shapes=[
                pltpu.VMEM((pieces, width, 2 * rank), jnp.bfloat16),
                pltpu.VMEM((2 * rank, width), jnp.bfloat16),
                pltpu.VMEM((rank, width), jnp.bfloat16),
            ],
        ),
        compiler_params=pltpu.CompilerParams(vmem_limit_bytes=14 * 2**20),
        name="finish",
    )(place, left, core, right, *[in_vmem(part) for part in held])


def blocked_body(*arguments):
    return blocked_steps(*arguments)


def blocked_steps(covariance, estimate, dual_var, start_basis):
    n_row, n_col = lax.axis_size("row"), lax.axis_size("col")
    lanes = n_row // n_col
    row_index, col_index = lax.axis_index("row"), lax.axis_index("col")
    lane, chip = row_index % lanes, row_index // lanes
    rows, columns = estimate.shape
    width = columns // n_row

    def across_lanes(value, step):
        route = [(r, r // lanes * lanes + (r % lanes ^ step)) for r in range(n_row)]
        return lax.ppermute(value, "row", route)

    def across_chips(value, step):
        route = [(r, (r // lanes ^ step) * lanes + r % lanes) for r in range(n_row)]
        return lax.ppermute(value, "row", route)

    def across_columns(value, step):
        return lax.ppermute(value, "col", [(c, c ^ step) for c in range(n_col)])

    def total_of(value, move, count):
        arrived = []
        for step in range(1, count):
            arrived.append(move(value, step))
        return sum(arrived, value)

    def block_at(step, s):
        return (lane ^ step) * n_col + (chip ^ s)

    calls = [[(step, s) for s in range(1, n_col)] for step in reversed(range(lanes))]
    calls.append([(step, 0) for step in reversed(range(lanes))])
    orders = [jnp.stack([block_at(*at) for at in call]).astype(jnp.int32) for call in calls]
    piece_rows = jnp.stack([col_index ^ a for a in range(n_col)]).astype(jnp.int32)
    corner = jnp.stack([row_index * rows, col_index * columns]).astype(jnp.int32)
    place = jnp.concatenate(orders + [piece_rows, piece_rows, corner])
    piece_rows = jnp.concatenate([piece_rows, lane.reshape(1).astype(jnp.int32)])
    local = jnp.broadcast_to(chip == col_index, (8, 128)).astype(jnp.float32)
    orders, piece_rows, place, local = lax.optimization_barrier((orders, piece_rows, place, local))

    part, high, held, basis = {}, [], [], in_hbm(start_basis)
    for index, call in enumerate(calls):
        if index == lanes:
            gathered = sum([part[step] for step in range(1, lanes)], part[0])
            gathered, orders[index] = lax.optimization_barrier((gathered, orders[index]))
        out = image_part(
            orders[index], estimate, dual_var, covariance, basis, len(call), width, index == 0
        )
        if index == 0:
            basis = out[3]
        high.append(out[1])
        held.append(out[2])
        step = call[0][0]
        if index < lanes:
            if step:
                part[step] = across_lanes(out[0], step)
            else:
                part[0] = out[0]
    last = out[0]
    own = last[lanes - 1]
    for index in range(lanes - 1):
        own = own + across_lanes(last[index], calls[-1][index][0])
    for s in range(1, n_col):
        arrived = across_chips(gathered[s - 1], s)
        own = own + arrived
    half = [own]
    for s in range(1, n_col):
        highest_step = 1 << (s.bit_length() - 1)
        half.append(across_chips(half[s - highest_step], highest_step))
    arrivals = []
    for a in range(n_col):
        route = [
            (r * n_col + c, (c * lanes + r % lanes) * n_col + (r // lanes ^ a))
            for r in range(n_row)
            for c in range(n_col)
            if r // lanes ^ a != c
        ]
        arrivals.append(lax.ppermute(own, ("row", "col"), route))
    right = {(0, s): half[s] for s in range(n_col)}
    for step in range(1, lanes):
        for s in range(n_col):
            right[step, s] = across_lanes(half[s], step)
    product = None
    for step in range(lanes):
        at = lanes - 1 - step
        product = product_part(
            [high[at], high[lanes]],
            (n_col - 1, 1),
            (0, at),
            [right[step, s] for s in range(1, n_col)] + [right[step, 0]],
            product,
        )
    local, product = lax.optimization_barrier((local, product))
    left = [jnp.where(local[:1, :1] > 0.5, half[a], arrivals[a]) for a in range(n_col)]
    shares = quadratic(piece_rows, left, product, lanes)
    both = sum([across_lanes(shares[step], step) for step in range(1, lanes)], shares[0])
    both = total_of(both, across_chips, n_col)
    small, gram = lax.optimization_barrier((both[0], both[1]))

    def of_lanes(share):
        return [share] + [across_lanes(share, step) for step in range(1, lanes)]

    grams = of_lanes(gram)
    inverse = factor_of(piece_rows, grams)
    small = total_of(small, across_columns, n_col)
    smalls = of_lanes(small)
    core = core_of(piece_rows, inverse, smalls)
    right_all = jnp.stack([right[at] for call in calls for at in call])
    return finish(place, jnp.stack(left), core, right_all, held)


def power_of_two(count):
    return count & (count - 1) == 0


def chosen_body(mesh):
    n_row, n_col = mesh.shape["row"], mesh.shape["col"]

    def pick(covariance, estimate, dual_var, start_basis):
        rows, columns = estimate.shape
        fits = n_row % n_col == 0 and power_of_two(n_row) and power_of_two(n_col)
        fits = fits and columns % (128 * n_row) == 0 and rows * n_row == columns * n_col
        fits = fits and start_basis.shape[1] % 128 == 0
        chosen = blocked_body if fits else body
        return chosen(covariance, estimate, dual_var, start_basis)

    return pick


def solution(mesh):
    return jax.shard_map(
        chosen_body(mesh),
        mesh=mesh,
        in_specs=(P("row", "col"), P("row", "col"), P("row", "col"), P("row", None)),
        out_specs=(P("row", "col"), P("row", "col")),
        check_vma=False,
    )
```

```python
import functools

import jax
import jax.numpy as jnp
from jax import lax
from jax.experimental import pallas as pl
from jax.experimental.pallas import tpu as pltpu
from jax.sharding import PartitionSpec as P


NS_ITERS = 12


penalty = 0.01
threshold = 0.2
base_level = 10.0
highest = lax.Precision.HIGHEST


def from_root(value, axis, source):
    kept = jnp.where(lax.axis_index(axis) == source, value, 0).astype(value.dtype)
    return lax.psum(kept, axis)


def inner_product(left_side, right_side):
    return lax.dot_general(
        left_side,
        right_side,
        (((0,), (0,)), ((), ())),
        precision=highest,
        preferred_element_type=jnp.float32,
    )


def normalize(mapped, gram_matrix):
    lower_factor = jnp.linalg.cholesky(gram_matrix)
    identity = jnp.eye(gram_matrix.shape[0], dtype=jnp.float32)
    inverse = lax.linalg.triangular_solve(lower_factor, identity, left_side=True, lower=True)
    return jnp.dot(mapped, inverse.T, precision=highest, preferred_element_type=jnp.float32)


def response_of(ritz_matrix):
    identity = jnp.eye(ritz_matrix.shape[0], dtype=jnp.float32)
    square = (
        jnp.dot(ritz_matrix, ritz_matrix, precision=highest, preferred_element_type=jnp.float32)
        + 4.0 * penalty * identity
    )
    frobenius = jnp.sqrt(jnp.sum(square * square))

    def newton(sweep_index, state_pair):
        iterate, partner = state_pair
        factor = 0.5 * (
            3.0 * identity
            - jnp.dot(partner, iterate, precision=highest, preferred_element_type=jnp.float32)
        )
        return (
            jnp.dot(iterate, factor, precision=highest, preferred_element_type=jnp.float32),
            jnp.dot(factor, partner, precision=highest, preferred_element_type=jnp.float32),
        )

    iterate, _ = lax.fori_loop(0, NS_ITERS, newton, (square / frobenius, identity))
    square_root = jnp.sqrt(frobenius) * iterate
    return (ritz_matrix + square_root) / (2.0 * penalty) - base_level * identity


def column_basis(shifted, row_basis):
    partial_terms = lax.dot_general(
        shifted,
        row_basis,
        (((0,), (0,)), ((), ())),
        precision=highest,
        preferred_element_type=jnp.float32,
    )
    mapped = lax.psum(partial_terms, "row")
    gram_matrix = lax.psum(inner_product(mapped, mapped), "col")
    return normalize(mapped, gram_matrix)


def row_image(shifted, col_basis):
    local_terms = jnp.dot(shifted, col_basis, precision=highest, preferred_element_type=jnp.float32)
    return lax.psum(local_terms, "col")


def row_inner(left_side, right_side):
    return lax.psum(inner_product(left_side, right_side), "row")


def body(covariance, estimate, dual_var, start_basis):
    shifted = penalty * (
        estimate.astype(jnp.float32) - dual_var.astype(jnp.float32)
    ) - covariance.astype(jnp.float32)
    rows_tile = shifted.shape[0]
    cols_tile = shifted.shape[1]
    row_basis = start_basis
    col_basis = column_basis(shifted, row_basis)
    blocks_per_column = lax.axis_size("row") // lax.axis_size("col")
    row_index = lax.axis_index("row")
    own_block = lax.dynamic_slice_in_dim(
        col_basis, row_index % blocks_per_column * rows_tile, rows_tile, 0
    )
    row_basis = from_root(own_block, "col", row_index // blocks_per_column)
    product = row_image(shifted, col_basis)
    raw_ritz = row_inner(row_basis, product)
    ritz_matrix = 0.5 * (raw_ritz + raw_ritz.T)
    response = response_of(ritz_matrix)
    weighted = jnp.dot(row_basis, response, precision=highest, preferred_element_type=jnp.float32)
    theta_tile = lax.dot_general(
        weighted,
        col_basis,
        (((1,), (1,)), ((), ())),
        precision=highest,
        preferred_element_type=jnp.float32,
    )
    row_ids = row_index * rows_tile + lax.broadcasted_iota(jnp.int32, (rows_tile, 1), 0)
    col_ids = lax.axis_index("col") * cols_tile + lax.broadcasted_iota(jnp.int32, (1, cols_tile), 1)
    theta_tile = theta_tile + jnp.where(row_ids == col_ids, base_level, 0.0)
    mixture = theta_tile + dual_var.astype(jnp.float32)
    clipped = jnp.clip(mixture, -threshold, threshold)
    return (mixture - clipped, clipped.astype(jnp.bfloat16))


def in_hbm(value):
    return pltpu.with_memory_space_constraint(value, pltpu.HBM)


def in_vmem(value):
    return pltpu.with_memory_space_constraint(value, pltpu.VMEM)


def split_two(value):
    high = value.astype(jnp.bfloat16)
    low = (value - high.astype(jnp.float32)).astype(jnp.bfloat16)
    return high, low


def contract(left_side, right_side, dims):
    return lax.dot_general(
        left_side, right_side, (dims, ((), ())), preferred_element_type=jnp.float32
    )


def image_kernel(order_ref, est_ref, dual_ref, cov_ref, basis_ref, *refs):
    part_ref, high_ref, held_ref, *more = refs
    step = pl.program_id(0)
    rows, width = est_ref.shape
    rank = part_ref.shape[1]
    stack_ref = basis_ref
    if more:
        stack_ref = more[0]

        @pl.when(step == 0)
        def _():
            high, low = split_two(basis_ref[...].T)
            stack_ref[:rank, :] = high
            stack_ref[rank:, :] = low

    depth = min(rows, 512)
    total = jnp.zeros((2 * rank, width), jnp.float32)
    extra = jnp.zeros((rank, width), jnp.float32)
    columns = pl.ds(pl.multiple_of(step * width, width), width)
    for start in range(0, rows, depth):
        span = slice(start, start + depth)
        dual_piece = dual_ref[span, :]
        shifted = penalty * (
            est_ref[span, :].astype(jnp.float32) - dual_piece.astype(jnp.float32)
        ) - cov_ref[span, :].astype(jnp.float32)
        high, low = split_two(shifted)
        high_ref[span, columns] = high
        held_ref[span, columns] = dual_piece
        total += contract(stack_ref[:, span], high, ((1,), (0,)))
        extra += contract(stack_ref[:rank, span], low, ((1,), (0,)))
    part_ref[0] = total[:rank] + total[rank:] + extra


def image_part(order, estimate, dual_var, covariance, basis, pieces, piece_width, first):
    rows = estimate.shape[0]
    rank = basis.shape[1] if first else basis.shape[0] // 2
    width = 256 if piece_width % 256 == 0 else 128
    per_piece = piece_width // width
    tile = pl.BlockSpec(
        (rows, width), lambda j, o: (0, o[j // per_piece] * per_piece + j % per_piece)
    )
    whole = pieces * piece_width
    vmem = pl.BlockSpec(memory_space=pltpu.VMEM)
    kept = pltpu.VMEM((rows, whole), jnp.bfloat16)
    stack = [jax.ShapeDtypeStruct((2 * rank, rows), jnp.bfloat16)] * first
    return pl.pallas_call(
        image_kernel,
        out_shape=(
            jax.ShapeDtypeStruct((pieces, rank, piece_width), jnp.float32), kept, kept, *stack
        ),
        grid_spec=pltpu.PrefetchScalarGridSpec(
            num_scalar_prefetch=1,
            grid=(pieces * per_piece,),
            in_specs=[tile, tile, tile, vmem],
            out_specs=[
                pl.BlockSpec((1, rank, width), lambda j, o: (j // per_piece, 0, j % per_piece)),
                vmem,
                vmem,
            ]
            + [vmem] * first,
        ),
        compiler_params=pltpu.CompilerParams(vmem_limit_bytes=14 * 2**20),
        name="image_part",
    )(order, in_hbm(estimate), in_hbm(dual_var), in_hbm(covariance), basis)


def product_kernel(*refs, counts, places, seeded):
    high_refs, refs = refs[: len(counts)], refs[len(counts) :]
    *piece_refs, out_ref, stack_ref = refs
    rows, rank = out_ref.shape
    if seeded:
        *piece_refs, prior_ref = piece_refs
    width = piece_refs[0].shape[1]
    for index, piece_ref in enumerate(piece_refs):
        high, low = split_two(piece_ref[...])
        stack_ref[:rank, index * width : (index + 1) * width] = high
        stack_ref[rank:, index * width : (index + 1) * width] = low
    depth = min(rows, 256)
    for start in range(0, rows, depth):
        span = slice(start, start + depth)
        both = jnp.zeros((depth, 2 * rank), jnp.float32)
        done = 0
        for high_ref, count, place in zip(high_refs, counts, places):
            there = slice(place * width, (place + count) * width)
            here = slice(done * width, (done + count) * width)
            both += contract(high_ref[span, there], stack_ref[:, here], ((1,), (1,)))
            done += count
        total = both[:, :rank] + both[:, rank:]
        out_ref[span, :] = prior_ref[span, :] + total if seeded else total


def product_part(highs, counts, places, pieces, prior=None):
    rows = highs[0].shape[0]
    rank, width = pieces[0].shape
    seeded = prior is not None
    vmem = pl.BlockSpec(memory_space=pltpu.VMEM)
    return pl.pallas_call(
        functools.partial(product_kernel, counts=counts, places=places, seeded=seeded),
        out_shape=jax.ShapeDtypeStruct((rows, rank), jnp.float32),
        in_specs=[vmem] * (len(highs) + len(pieces) + seeded),
        out_specs=vmem,
        scratch_shapes=[pltpu.VMEM((2 * rank, width * len(pieces)), jnp.bfloat16)],
        compiler_params=pltpu.CompilerParams(vmem_limit_bytes=12 * 2**20),
        name="product_part",
    )(*[in_vmem(high) for high in highs], *pieces, *([prior] * seeded))


def dot_three(left_side, right_side, dims=((1,), (0,))):
    left_high, left_low = split_two(left_side)
    right_high, right_low = split_two(right_side)
    return (
        contract(left_high, right_high, dims)
        + contract(left_low, right_high, dims)
        + contract(left_high, right_low, dims)
    )


def quadratic_kernel(where_ref, *refs):
    *piece_refs, product_ref, out_ref, small_ref, gram_ref = refs
    count = len(piece_refs) // 2
    rank, width = piece_refs[0].shape
    small = jnp.zeros((rank, rank), jnp.float32)
    gram = jnp.zeros((rank, rank), jnp.float32)
    own_block = where_ref[count + 1] > 0
    for index in range(count):
        start = pl.multiple_of(where_ref[index] * width, width)
        piece = jnp.where(own_block, piece_refs[index][...], piece_refs[count + index][...])
        small += dot_three(piece, product_ref[pl.ds(start, width), :])
        gram += dot_three(piece, piece, ((1,), (1,)))
    small_ref[...] = small
    gram_ref[...] = gram
    lanes, _, share, _ = out_ref.shape
    for step in range(lanes):
        start = pl.multiple_of((where_ref[count] ^ step) * share, share)
        out_ref[step, 0] = small_ref[pl.ds(start, share), :]
        out_ref[step, 1] = gram_ref[pl.ds(start, share), :]


def quadratic(order, here, arrived, product, lanes):
    rank = product.shape[1]
    vmem = pl.BlockSpec(memory_space=pltpu.VMEM)
    return pl.pallas_call(
        quadratic_kernel,
        out_shape=jax.ShapeDtypeStruct((lanes, 2, rank // lanes, rank), jnp.float32),
        in_specs=[pl.BlockSpec(memory_space=pltpu.SMEM)] + [vmem] * (2 * len(here) + 1),
        out_specs=vmem,
        scratch_shapes=[pltpu.VMEM((rank, rank), jnp.float32)] * 2,
        compiler_params=pltpu.CompilerParams(vmem_limit_bytes=8 * 2**20),
        name="quadratic",
    )(order, *here, *arrived, product)


def joined(where_ref, share_refs, whole_ref):
    share = share_refs[0].shape[0]
    lane = where_ref[where_ref.shape[0] - 1]
    for step, share_ref in enumerate(share_refs):
        start = pl.multiple_of((lane ^ step) * share, share)
        whole_ref[pl.ds(start, share), :] = share_ref[...]


def spread_row(band, index):
    return jnp.broadcast_to(band[index : index + 1, :], band.shape)


def spread_column(band, index):
    return jnp.broadcast_to(band[:, index : index + 1], band.shape)


def factor_kernel(where_ref, *refs):
    *share_refs, out_ref, gram_ref = refs
    joined(where_ref, share_refs, gram_ref)
    rank = gram_ref.shape[0]
    look = 8
    bands = rank // 8
    sublanes = lax.broadcasted_iota(jnp.int32, (8, rank), 0)
    lanes = lax.broadcasted_iota(jnp.int32, (8, rank), 1)
    left = [gram_ref[8 * i : 8 * i + 8, :] for i in range(bands)]
    right = [jnp.where(lanes == sublanes + 8 * i, 1.0, 0.0).astype(jnp.float32) for i in range(bands)]
    for start in range(0, rank, look):
        band, offset = start // 8, start % 8
        rows = [spread_row(left[band], offset + t) for t in range(look)]
        others = [spread_row(right[band], offset + t) for t in range(look)]
        small = [[spread_column(rows[t], start + u) for u in range(t + 1)] for t in range(look)]
        ratio = [[None] * look for _ in range(look)]
        scale = [None] * look
        for t in range(look):
            scale[t] = 1.0 / small[t][t]
            for v in range(t + 1, look):
                ratio[v][t] = small[v][t] * scale[t]
                for w in range(t + 1, v + 1):
                    small[v][w] = small[v][w] - ratio[v][t] * small[w][t]
                rows[v] = rows[v] - ratio[v][t] * rows[t]
                others[v] = others[v] - ratio[v][t] * others[t]
        for i in range(band, bands):
            columns = []
            for t in range(look):
                column = spread_column(left[i], start + t)
                for u in range(t):
                    column = column - ratio[t][u] * columns[u]
                columns.append(column)
            update, other = left[i], right[i]
            for t in range(look):
                amount = columns[t] * scale[t]
                update = update - amount * rows[t]
                other = other - amount * others[t]
            if i == band:
                final, final_other = left[i], right[i]
                for t in range(look):
                    root = lax.rsqrt(small[t][t])
                    final_other = jnp.where(sublanes == offset + t, others[t] * root, final_other)
                other = jnp.where(sublanes >= offset + look, other, final_other)
                update = jnp.where(sublanes >= offset + look, update, final)
            left[i], right[i] = update, other
    for i in range(bands):
        out_ref[8 * i : 8 * i + 8, :] = right[i]


def factor_of(order, shares):
    rank = shares[0].shape[1]
    vmem = pl.BlockSpec(memory_space=pltpu.VMEM)
    return pl.pallas_call(
        factor_kernel,
        out_shape=jax.ShapeDtypeStruct((rank, rank), jnp.float32),
        in_specs=[pl.BlockSpec(memory_space=pltpu.SMEM)] + [vmem] * len(shares),
        out_specs=vmem,
        scratch_shapes=[pltpu.VMEM((rank, rank), jnp.float32)],
        compiler_params=pltpu.CompilerParams(vmem_limit_bytes=4 * 2**20),
        name="factor",
    )(order, *shares)


def core_kernel(where_ref, inverse_ref, *refs):
    *share_refs, out_ref, small_ref = refs
    joined(where_ref, share_refs, small_ref)
    rank = small_ref.shape[0]
    row_ids = lax.broadcasted_iota(jnp.int32, (rank, rank), 0)
    col_ids = lax.broadcasted_iota(jnp.int32, (rank, rank), 1)
    identity = jnp.where(row_ids == col_ids, 1.0, 0.0).astype(jnp.float32)
    inverse = inverse_ref[...]
    raw = dot_three(dot_three(inverse, small_ref[...]), inverse, ((1,), (1,)))
    ritz = 0.5 * (raw + raw.T)
    square = dot_three(ritz, ritz) + 4.0 * penalty * identity
    frobenius = jnp.sqrt(jnp.sum(jnp.sum(square * square, axis=1, keepdims=True), axis=0, keepdims=True))

    def product(left_high, left_low, right_high, right_low):
        wide = jnp.concatenate([left_high, left_low], axis=1)
        twice = jnp.concatenate([right_high, right_high], axis=0)
        flat = ((1,), (0,))
        return contract(wide, twice, flat) + contract(left_high, right_low, flat)

    def newton(_, pair):
        iterate, partner = pair
        iterate_parts, partner_parts = split_two(iterate), split_two(partner)
        factor = 0.5 * (3.0 * identity - product(*partner_parts, *iterate_parts))
        factor_parts = split_two(factor)
        return product(*iterate_parts, *factor_parts), product(*factor_parts, *partner_parts)

    iterate, _ = lax.fori_loop(0, NS_ITERS, newton, (square / frobenius, identity))
    root = jnp.sqrt(frobenius) * iterate
    response = (ritz + root) / (2.0 * penalty) - base_level * identity
    out_ref[...] = dot_three(dot_three(inverse, response, ((0,), (0,))), inverse)


def core_of(order, inverse, shares):
    vmem = pl.BlockSpec(memory_space=pltpu.VMEM)
    return pl.pallas_call(
        core_kernel,
        out_shape=jax.ShapeDtypeStruct(inverse.shape, jnp.float32),
        in_specs=[pl.BlockSpec(memory_space=pltpu.SMEM)] + [vmem] * (1 + len(shares)),
        out_specs=vmem,
        scratch_shapes=[pltpu.VMEM(inverse.shape, jnp.float32)],
        compiler_params=pltpu.CompilerParams(vmem_limit_bytes=8 * 2**20),
        name="core",
    )(order, inverse, *shares)


def finish_kernel(place_ref, left_ref, core_ref, right_ref, *refs, groups, pieces, counts):
    *held_refs, est_ref, dual_ref, left_stack, right_twice, right_low = refs
    group = pl.program_id(0)
    piece = pl.program_id(1)
    height, width = est_ref.shape
    rank = core_ref.shape[0]

    @pl.when(group == 0)
    def _():
        weighted = dot_three(left_ref[0], core_ref[...], ((0,), (0,)))
        high, low = split_two(weighted)
        left_stack[piece, :, :rank] = high
        left_stack[piece, :, rank:] = low

    @pl.when(piece == 0)
    def _():
        high, low = split_two(right_ref[0])
        right_twice[:rank, :] = high
        right_twice[rank:, :] = high
        right_low[...] = low

    rows = pl.ds(pl.multiple_of(place_ref[groups + piece] * height, height), height)
    first, held = 0, None
    for held_ref, count in zip(held_refs, counts):
        at = jnp.clip(group - first, 0, count - 1)
        block = held_ref[rows, pl.ds(pl.multiple_of(at * width, width), width)]
        held = block if held is None else jnp.where(group >= first, block, held)
        first += count
    theta = contract(left_stack[piece], right_twice[...], ((1,), (0,)))
    theta += contract(left_stack[piece, :, :rank], right_low[...], ((1,), (0,)))
    row_ids = place_ref[groups + 2 * pieces] + place_ref[groups + piece] * height
    col_ids = place_ref[groups + 2 * pieces + 1] + place_ref[group] * width
    row_ids = row_ids + lax.broadcasted_iota(jnp.int32, (height, 1), 0)
    col_ids = col_ids + lax.broadcasted_iota(jnp.int32, (1, width), 1)
    theta = theta + jnp.where(row_ids == col_ids, base_level, 0.0)
    mixture = theta + held.astype(jnp.float32)
    clipped = jnp.clip(mixture, -threshold, threshold)
    est_ref[...] = mixture - clipped
    dual_ref[...] = clipped.astype(jnp.bfloat16)


def finish(place, left, core, right, held):
    pieces, rank, width = left.shape
    groups = right.shape[0]
    rows = pieces * width
    columns = groups * width
    vmem = pl.BlockSpec(memory_space=pltpu.VMEM)
    tile = pl.BlockSpec((width, width), lambda g, a, p: (p[groups + a], p[g]))
    return pl.pallas_call(
        functools.partial(
            finish_kernel, groups=groups, pieces=pieces, counts=[h.shape[1] // width for h in held]
        ),
        out_shape=(
            jax.ShapeDtypeStruct((rows, columns), jnp.float32),
            jax.ShapeDtypeStruct((rows, columns), jnp.bfloat16),
        ),
        grid_spec=pltpu.PrefetchScalarGridSpec(
            num_scalar_prefetch=1,
            grid=(groups, pieces),
            in_specs=[
                pl.BlockSpec((1, rank, width), lambda g, a, p: (jnp.where(g == 0, a, 0), 0, 0)),
                vmem,
                pl.BlockSpec((1, rank, width), lambda g, a, p: (g, 0, 0)),
            ]
            + [vmem] * len(held),
            out_specs=[tile, tile],
            scratch_shapes=[
                pltpu.VMEM((pieces, width, 2 * rank), jnp.bfloat16),
                pltpu.VMEM((2 * rank, width), jnp.bfloat16),
                pltpu.VMEM((rank, width), jnp.bfloat16),
            ],
        ),
        compiler_params=pltpu.CompilerParams(vmem_limit_bytes=14 * 2**20),
        name="finish",
    )(place, left, core, right, *[in_vmem(part) for part in held])


def blocked_body(*arguments):
    return blocked_steps(*arguments)


def blocked_steps(covariance, estimate, dual_var, start_basis):
    n_row, n_col = lax.axis_size("row"), lax.axis_size("col")
    lanes = n_row // n_col
    row_index, col_index = lax.axis_index("row"), lax.axis_index("col")
    lane, chip = row_index % lanes, row_index // lanes
    rows, columns = estimate.shape
    width = columns // n_row

    def across_lanes(value, step):
        route = [(r, r // lanes * lanes + (r % lanes ^ step)) for r in range(n_row)]
        return lax.ppermute(value, "row", route)

    def across_chips(value, step):
        route = [(r, (r // lanes ^ step) * lanes + r % lanes) for r in range(n_row)]
        return lax.ppermute(value, "row", route)

    def across_columns(value, step):
        return lax.ppermute(value, "col", [(c, c ^ step) for c in range(n_col)])

    def total_of(value, move, count):
        arrived = []
        for step in range(1, count):
            arrived.append(move(value, step))
        return sum(arrived, value)

    def block_at(step, s):
        return (lane ^ step) * n_col + (chip ^ s)

    calls = [[(step, s) for s in range(1, n_col)] for step in reversed(range(lanes))]
    calls.append([(step, 0) for step in reversed(range(lanes))])
    orders = [jnp.stack([block_at(*at) for at in call]).astype(jnp.int32) for call in calls]
    piece_rows = jnp.stack([col_index ^ a for a in range(n_col)]).astype(jnp.int32)
    corner = jnp.stack([row_index * rows, col_index * columns]).astype(jnp.int32)
    place = jnp.concatenate(orders + [piece_rows, piece_rows, corner])
    piece_rows = jnp.concatenate([piece_rows, lane.reshape(1).astype(jnp.int32)])
    local = jnp.broadcast_to(chip == col_index, (1, 1)).astype(jnp.float32)
    spots = jnp.concatenate([piece_rows, (chip == col_index).reshape(1).astype(jnp.int32)])
    orders, piece_rows, place, local, spots = lax.optimization_barrier(
        (orders, piece_rows, place, local, spots)
    )

    part, high, held, basis = {}, [], [], in_hbm(start_basis)
    for index, call in enumerate(calls):
        if index == lanes:
            gathered = sum([part[step] for step in range(1, lanes)], part[0])
            gathered, orders[index] = lax.optimization_barrier((gathered, orders[index]))
        out = image_part(
            orders[index], estimate, dual_var, covariance, basis, len(call), width, index == 0
        )
        if index == 0:
            basis = out[3]
        high.append(out[1])
        held.append(out[2])
        step = call[0][0]
        if index < lanes:
            if step:
                part[step] = across_lanes(out[0], step)
            else:
                part[0] = out[0]
    last = out[0]
    own = last[lanes - 1]
    for index in range(lanes - 1):
        own = own + across_lanes(last[index], calls[-1][index][0])
    for s in range(1, n_col):
        arrived = across_chips(gathered[s - 1], s)
        own = own + arrived
    half = [own]
    for s in range(1, n_col):
        highest_step = 1 << (s.bit_length() - 1)
        half.append(across_chips(half[s - highest_step], highest_step))
    arrivals = []
    for a in range(n_col):
        route = [
            (r * n_col + c, (c * lanes + r % lanes) * n_col + (r // lanes ^ a))
            for r in range(n_row)
            for c in range(n_col)
            if r // lanes ^ a != c
        ]
        arrivals.append(lax.ppermute(own, ("row", "col"), route))
    right = {(0, s): half[s] for s in range(n_col)}
    for step in range(1, lanes):
        for s in range(n_col):
            right[step, s] = across_lanes(half[s], step)
    product = None
    for step in range(lanes):
        at = lanes - 1 - step
        product = product_part(
            [high[at], high[lanes]],
            (n_col - 1, 1),
            (0, at),
            [right[step, s] for s in range(1, n_col)] + [right[step, 0]],
            product,
        )
    shares = quadratic(spots, half, arrivals, product, lanes)
    both = sum([across_lanes(shares[step], step) for step in range(1, lanes)], shares[0])
    both = total_of(both, across_chips, n_col)
    small, gram, local = lax.optimization_barrier((both[0], both[1], local))
    left = [jnp.where(local > 0.5, half[a], arrivals[a]) for a in range(n_col)]

    def of_lanes(share):
        return [share] + [across_lanes(share, step) for step in range(1, lanes)]

    grams = of_lanes(gram)
    inverse = factor_of(piece_rows, grams)
    small = total_of(small, across_columns, n_col)
    smalls = of_lanes(small)
    core = core_of(piece_rows, inverse, smalls)
    right_all = jnp.stack([right[at] for call in calls for at in call])
    return finish(place, jnp.stack(left), core, right_all, held)


def power_of_two(count):
    return count & (count - 1) == 0


def chosen_body(mesh):
    n_row, n_col = mesh.shape["row"], mesh.shape["col"]

    def pick(covariance, estimate, dual_var, start_basis):
        rows, columns = estimate.shape
        fits = n_row % n_col == 0 and power_of_two(n_row) and power_of_two(n_col)
        fits = fits and columns % (128 * n_row) == 0 and rows * n_row == columns * n_col
        fits = fits and start_basis.shape[1] % 128 == 0
        chosen = blocked_body if fits else body
        return chosen(covariance, estimate, dual_var, start_basis)

    return pick


def solution(mesh):
    return jax.shard_map(
        chosen_body(mesh),
        mesh=mesh,
        in_specs=(P("row", "col"), P("row", "col"), P("row", "col"), P("row", None)),
        out_specs=(P("row", "col"), P("row", "col")),
        check_vma=False,
    )
```
